32 devices in a mesh: dp: 1, sp: 32 (over x, y, z, core).
Axes of the slice: x: 2, y: 2, z: 4, core: 2. Of those that a mesh axis runs over, the one named last changes fastest.
Arguments:
- x: bfloat16 [4096, 4096], P(('dp', 'sp'))
- gain: bfloat16 [4096], replicated
- wq: bfloat16 [4096, 4096], replicated
- wk: bfloat16 [4096, 1024], replicated
- wv: bfloat16 [4096, 1024], replicated
- wo: bfloat16 [4096, 4096], replicated
Outputs:
- output: bfloat16 [4096, 4096], P(('dp', 'sp'))
All inputs are finite; a program needn't handle non-finite values.
Results may differ from the reference program's by a relative error of at most 0.012.
Values are sent between devices in bfloat16 or wider.
A program may use at most 2 GiB of HBM per device.

```python
import jax
import jax.numpy as jnp
from jax import lax

ROWS = 4096
D = 4096
HEADS = 32
KV_HEADS = 8
HEAD = 128
THETA = 10000


def setup_inputs(seed: int = 0, part: int = 0) -> dict:
    kx, kn, kq, kk, kv, ko = jax.random.split(jax.random.key(seed), 6)

    def weights(key, rows, columns):
        return jax.random.normal(key, (rows, columns), jnp.float32) * rows**-0.5

    drawn = {
        "x": jax.random.normal(jax.random.fold_in(kx, part), (ROWS, D), jnp.float32),
        "gain": 1 + 0.1 * jax.random.normal(kn, (D,), jnp.float32),
        "wq": 2 * weights(kq, D, HEADS * HEAD),
        "wk": 2 * weights(kk, D, KV_HEADS * HEAD),
        "wv": 4 * weights(kv, D, KV_HEADS * HEAD),
        "wo": weights(ko, HEADS * HEAD, D),
    }
    return {k: v.astype(jnp.bfloat16) for k, v in drawn.items()}


def normed(x, gain):
    wide = x.astype(jnp.float32)
    scale = lax.rsqrt(jnp.mean(wide * wide, -1, keepdims=True) + 1e-6)
    return (wide * scale * gain.astype(jnp.float32)).astype(jnp.bfloat16)


def turned(t, place, theta):
    half = t.shape[-1] // 2
    angle = place.astype(jnp.float32)[:, None] * theta ** (-jnp.arange(half, dtype=jnp.float32) / half)
    cos, sin = jnp.cos(angle)[:, None], jnp.sin(angle)[:, None]
    a, b = t[..., :half].astype(jnp.float32), t[..., half:].astype(jnp.float32)
    return jnp.concatenate([a * cos - b * sin, b * cos + a * sin], -1).astype(jnp.bfloat16)


def matmul(a, w):
    return jnp.dot(a, w, preferred_element_type=jnp.float32).astype(jnp.bfloat16)


def einsum(form, a, b):
    return jnp.einsum(form, a.astype(jnp.float32), b.astype(jnp.float32))


def attention(q, k, v):
    scores = einsum("tgsd,ugd->gstu", q, k) * q.shape[-1] ** -0.5
    token = jnp.arange(q.shape[0])
    scores = jnp.where(token[:, None] >= token, scores, -jnp.inf)
    weights = jax.nn.softmax(scores, -1).astype(jnp.bfloat16)
    return einsum("gstu,ugd->tgsd", weights, v).astype(jnp.bfloat16)


def reference(x, gain, wq, wk, wv, wo):
    a, place = normed(x, gain), jnp.arange(ROWS)
    q = turned(matmul(a, wq).reshape(ROWS, HEADS, HEAD), place, THETA).reshape(ROWS, KV_HEADS, -1, HEAD)
    k = turned(matmul(a, wk).reshape(ROWS, KV_HEADS, HEAD), place, THETA)
    v = matmul(a, wv).reshape(ROWS, KV_HEADS, HEAD)
    seen = attention(q, k, v).reshape(ROWS, HEADS * HEAD)
    return (x.astype(jnp.float32) + jnp.dot(seen, wo, preferred_element_type=jnp.float32)).astype(jnp.bfloat16)
```

```python
import jax
import jax.numpy as jnp
from jax import lax
from jax.experimental import pallas as pl
from jax.experimental.pallas import tpu as pltpu
from jax.sharding import PartitionSpec as P

HEAD = 128
THETA = 10000
NEG = -1e30
HIDDEN = 2 * NEG
LOG2E = 1.4426950408889634
E = HEAD**-0.5 * LOG2E
F32, BF16 = jnp.float32, jnp.bfloat16
MESH = pl.DeviceIdType.MESH

OWN = 128
CHIP = 256
D = 4096
G = 4
COLS = G * CHIP
PIECE = 512
STRIP = 512
SUM = HEAD + 8


def _dot(a, b, ca=1, cb=0):
    return lax.dot_general(a, b, (((ca,), (cb,)), ((), ())), preferred_element_type=F32)


def _kernel(x_hbm, gain, cos, sin, wq, wk, wv, wo, y_hbm, w, xs, a, kvs, kv, qs, qr, top, mix, gap, os, orr, acc, out,
            xl_sem, w_sem, wo_sem, xs_sem, xr_sem, kvp_s, kv_r, up_s, dn_s, q_s, q_r, o_s, o_r, y_sem):
    dev = lax.axis_index("sp")
    c = lax.rem(dev, 2)
    z = lax.rem(lax.div(dev, 2), 4)
    p = lax.div(dev, 8)
    px, py = lax.div(p, 2), lax.rem(p, 2)

    def at(pp, zz, cc):
        return pp * 8 + zz * 2 + cc

    def flip(d):
        dx, dy = d // 2 if isinstance(d, int) else lax.div(d, 2), d % 2 if isinstance(d, int) else lax.rem(d, 2)
        return (px + dx - 2 * px * dx) * 2 + (py + dy - 2 * py * dy)

    def send(src, dst, ss, rs, to):
        return pltpu.make_async_remote_copy(src_ref=src, dst_ref=dst, send_sem=ss, recv_sem=rs, device_id={"sp": to}, device_id_type=MESH)

    partner = at(p, z, 1 - c)
    mine = pl.multiple_of(c * OWN, OWN)
    theirs = pl.multiple_of((1 - c) * OWN, OWN)
    cut = pl.multiple_of(c * PIECE, PIECE)

    x_load = pltpu.make_async_copy(x_hbm, xs.at[pl.ds(mine, OWN), :], xl_sem)
    x_load.start()
    wk_load = pltpu.make_async_copy(wk.at[:, pl.ds(cut, PIECE)], w.at[0], w_sem.at[0])
    wv_load = pltpu.make_async_copy(wv.at[:, pl.ds(cut, PIECE)], w.at[1], w_sem.at[1])
    wk_load.start()
    wv_load.start()

    def q_load(i):
        d = (3, 1, 2, 0)[i]
        col = pl.multiple_of((c * 4 + flip(d)) * PIECE, PIECE)
        return pltpu.make_async_copy(wq.at[:, pl.ds(col, PIECE)], w.at[2 + i], w_sem.at[2 + i])

    def wo_load(n):
        return pltpu.make_async_copy(wo.at[:, n * PIECE : (n + 1) * PIECE], w.at[(n + 6) % 8], wo_sem.at[n])

    barrier = pltpu.get_barrier_semaphore()

    def greet(to):
        pl.semaphore_signal(barrier, inc=1, device_id={"sp": to}, device_id_type=MESH)

    greet(partner)
    for d in (1, 2, 3):
        greet(at(flip(d), z, c))
        greet(at(flip(d), z, 1 - c))

    @pl.when(z > 0)
    def _():
        greet(dev - 2)

    @pl.when(z < 3)
    def _():
        greet(dev + 2)

    mix[...] = jnp.zeros_like(mix)
    top[...] = jnp.full_like(top, NEG)
    gap[...] = lax.rem(lax.broadcasted_iota(jnp.int32, (CHIP, STRIP), 1), CHIP) - lax.broadcasted_iota(jnp.int32, (CHIP, STRIP), 0)

    x_load.wait()

    @pl.when((z > 0) & (z < 3))
    def _():
        pl.semaphore_wait(barrier, 9)

    @pl.when((z == 0) | (z == 3))
    def _():
        pl.semaphore_wait(barrier, 8)

    x_send = send(xs.at[pl.ds(mine, OWN), :], xs.at[pl.ds(mine, OWN), :], xs_sem, xr_sem, partner)
    x_send.start()

    def norm(first):
        def rows(i, _):
            here = pl.ds(pl.multiple_of(first + i * 16, 16), 16)
            wide = xs[here, :].astype(F32)
            scale = lax.rsqrt(jnp.mean(wide * wide, -1, keepdims=True) + 1e-6)
            a[here, :] = (wide * scale * gain[...].astype(F32)).astype(BF16)
            return 0

        lax.fori_loop(0, OWN // 16, rows, 0)

    norm(mine)
    send(xs.at[pl.ds(theirs, OWN), :], xs.at[pl.ds(theirs, OWN), :], xs_sem, xr_sem, partner).wait_recv()
    norm(theirs)

    def turned(h):
        h = h.astype(BF16).astype(F32)
        return (h * cos[...] + pltpu.roll(h, HEAD // 2, 1) * sin[...]).astype(BF16)

    wk_load.wait()
    for i in range(4):
        q_load(i).start()
    wo_load(0).start()
    wo_load(1).start()
    t = _dot(a[...], w[0])
    for j in range(4):
        kvs[j, :CHIP, :] = turned(t[:, j * HEAD : (j + 1) * HEAD])
    wv_load.wait()
    t = _dot(a[...], w[1])
    for j in range(4):
        for n in range(2):
            kvs[j, CHIP + n * HEAD : CHIP + (n + 1) * HEAD, :] = t[n * HEAD : (n + 1) * HEAD, j * HEAD : (j + 1) * HEAD].T.astype(BF16)
    wo_load(2).start()
    wo_load(3).start()

    own_slot = p * 4 + z
    plane = [send(kvs.at[flip(d)], kv.at[own_slot], kvp_s.at[d - 1], kv_r.at[own_slot], at(flip(d), z, c)) for d in (1, 2, 3)]
    for s in plane:
        s.start()
    kv[own_slot] = kvs[p]

    def up(s):
        return send(kv.at[s], kv.at[s], up_s.at[s], kv_r.at[s], dev + 2)

    def down(s):
        return send(kv.at[s], kv.at[s], dn_s.at[s], kv_r.at[s], dev - 2)

    def pass_up(s):
        @pl.when(z < 3)
        def _():
            up(s).start()

    def pass_down(s, b):
        @pl.when((z > 0) & (b < 3))
        def _():
            down(s).start()

    def arrived(s):
        send(kv.at[s], kv.at[s], up_s.at[s], kv_r.at[s], partner).wait_recv()

    pass_up(own_slot)
    pass_down(own_slot, p)

    for i in range(4):
        d = (3, 1, 2, 0)[i]
        q_load(i).wait()
        t = _dot(a[...], w[2 + i])
        dst = qr.at[p] if d == 0 else qs.at[d]
        for g in range(G):
            dst[g * CHIP : (g + 1) * CHIP, :] = turned(t[:, g * HEAD : (g + 1) * HEAD])
        if d:
            send(qs.at[d], qr.at[p], q_s.at[d - 1], q_r.at[p], at(flip(d), z, c)).start()
        wo_load(4 + i).start()

    for d in (1, 2, 3):
        s = flip(d) * 4 + z
        arrived(s)
        pass_up(s)
        pass_down(s, flip(d))

    ones = jnp.ones((8, CHIP), BF16)

    def item(b, s, masked):
        k = kv[s, :CHIP, :]
        values = jnp.concatenate([jnp.concatenate([kv[s, CHIP : CHIP + HEAD, :], kv[s, CHIP + HEAD :, :]], axis=1), ones], axis=0)
        strips = range(0, COLS, STRIP)
        scores = [_dot(k, qr[b, i : i + STRIP, :], 1, 1) for i in strips]
        weights, keeps = [], []
        for i, v in zip(strips, scores):
            if masked:
                v = jnp.where(gap[...] >= 0, v, HIDDEN)
            old = top[b, 0:1, i : i + STRIP]
            new = jnp.maximum(old, v.max(axis=0, keepdims=True))
            top[b, 0:1, i : i + STRIP] = new
            weights.append(jnp.exp2((v - new) * E).astype(BF16))
            keeps.append(jnp.exp2((old - new) * E))
        for i, v, keep in zip(strips, weights, keeps):
            mix[b, :, i : i + STRIP] = mix[b, :, i : i + STRIP] * keep + _dot(values, v)

    def come(b, u, far):
        there = jnp.where(u == 0, z >= far, (z + far <= 3) & (b < 3))
        return there, b * 4 + jnp.where(u == 0, z - far, z + far)

    def take(b, far):
        for u in range(2):
            there, s = come(b, u, far)

            @pl.when(there)
            def _():
                arrived(s)
                if u == 0:
                    pass_up(s)
                else:
                    pass_down(s, b)

    def near(i, _):
        b = flip(i)

        @pl.when(i == 2)
        def _():
            lax.fori_loop(0, 4, lambda n, _: (take(n, 1), 0)[1], 0)

        @pl.when(i > 0)
        def _():
            send(qs.at[0], qr.at[b], q_s.at[0], q_r.at[b], partner).wait_recv()

        item(b, b * 4 + z, True)
        lax.fori_loop(0, b, lambda n, _: (item(b, n * 4 + z, False), 0)[1], 0)
        return 0

    lax.fori_loop(0, 4, near, 0)

    def finish(b):
        total = mix[b, HEAD : HEAD + 1, :]
        o = mix[b, :HEAD, :] * (1 / total)
        for g in range(G):
            for h in range(2):
                os[b, h, :, g * HEAD : (g + 1) * HEAD] = o[:, g * CHIP + h * OWN : g * CHIP + (h + 1) * OWN].T.astype(BF16)
        for h in range(2):
            to = at(b, z, h)

            @pl.when(to != dev)
            def _():
                send(os.at[b, h], orr.at[c * 4 + p], o_s.at[b, h], o_r.at[c * 4 + p], to).start()

            @pl.when(to == dev)
            def _():
                orr[c * 4 + p] = os[b, h]

    def step(n, _):
        far, b = lax.div(n, 4) + 1, lax.rem(n, 4)

        @pl.when(far == 3)
        def _():
            take(b, 3)

        def way(u, _):
            there, s = come(b, u, far)

            @pl.when(there)
            def _():
                lax.fori_loop(b + u, 4, lambda m, _: (item(m, s, False), 0)[1], 0)

            return 0

        lax.fori_loop(0, 2, way, 0)

        @pl.when(far == 1)
        def _():
            take(b, 2)

        @pl.when(far == 3)
        def _():
            finish(b)

        return 0

    lax.fori_loop(0, 12, step, 0)

    for n in range(8):
        wo_load(n).wait()

    def project(d, _):
        pp = flip(d)
        for cc in range(2):
            j = cc * 4 + pp

            @pl.when(at(pp, z, cc) != dev)
            def _():
                send(os.at[0, 0], orr.at[j], o_s.at[0, 0], o_r.at[j], partner).wait_recv()

        for n in range(8):
            here = slice(n * PIECE, (n + 1) * PIECE)
            t = acc[:, here]
            for cc in range(2):
                j = cc * 4 + pp
                t = t + _dot(orr[j], w[(n + 6) % 8, pl.ds(pl.multiple_of(j * PIECE, PIECE), PIECE), :])
            acc[:, here] = t
        return 0

    acc[...] = xs[pl.ds(mine, OWN), :].astype(F32)
    lax.fori_loop(0, 4, project, 0)
    out[...] = acc[...].astype(BF16)
    y_store = pltpu.make_async_copy(out, y_hbm, y_sem)
    y_store.start()

    x_send.wait_send()
    for s in plane:
        s.wait_send()
    for d in (1, 2, 3):
        send(qs.at[d], qr.at[p], q_s.at[d - 1], q_r.at[p], partner).wait_send()

    def left(s, _):
        zz, b = lax.rem(s, 4), lax.div(s, 4)

        @pl.when((z < 3) & (zz <= z))
        def _():
            up(s).wait_send()

        @pl.when((z > 0) & (zz >= z) & (b < 3))
        def _():
            down(s).wait_send()

        return 0

    lax.fori_loop(0, 16, left, 0)

    for b in range(4):
        for h in range(2):

            @pl.when(at(b, z, h) != dev)
            def _():
                send(os.at[b, h], orr.at[0], o_s.at[b, h], o_r.at[0], partner).wait_send()

    y_store.wait()


def solution(mesh):
    def step(x, gain, wq, wk, wv, wo):
        place = lax.div(lax.axis_index("sp"), 2) * CHIP + jnp.arange(CHIP)
        half = HEAD // 2
        angle = place.astype(F32)[:, None] * THETA ** (-jnp.arange(half, dtype=F32) / half)
        cos, sin = jnp.cos(angle), jnp.sin(angle)
        cos, sin = jnp.concatenate([cos, cos], -1), jnp.concatenate([-sin, sin], -1)
        vmem, hbm = pl.BlockSpec(memory_space=pltpu.VMEM), pl.BlockSpec(memory_space=pl.ANY)
        dma = pltpu.SemaphoreType.DMA
        return pl.pallas_call(
            _kernel,
            out_shape=jax.ShapeDtypeStruct((OWN, D), BF16),
            in_specs=[hbm, vmem, vmem, vmem, hbm, hbm, hbm, hbm],
            out_specs=hbm,
            scratch_shapes=[
                pltpu.VMEM((8, D, PIECE), BF16),
                pltpu.VMEM((CHIP, D), BF16),
                pltpu.VMEM((CHIP, D), BF16),
                pltpu.VMEM((4, 2 * CHIP, HEAD), BF16),
                pltpu.VMEM((16, 2 * CHIP, HEAD), BF16),
                pltpu.VMEM((4, COLS, HEAD), BF16),
                pltpu.VMEM((4, COLS, HEAD), BF16),
                pltpu.VMEM((4, 8, COLS), F32),
                pltpu.VMEM((4, SUM, COLS), F32),
                pltpu.VMEM((CHIP, STRIP), jnp.int32),
                pltpu.VMEM((4, 2, OWN, PIECE), BF16),
                pltpu.VMEM((8, OWN, PIECE), BF16),
                pltpu.VMEM((OWN, D), F32),
                pltpu.VMEM((OWN, D), BF16),
                dma, dma((6,)), dma((8,)), dma, dma, dma((3,)), dma((16,)), dma((16,)), dma((16,)), dma((3,)), dma((4,)),
                dma((4, 2)), dma((8,)), dma,
            ],
            compiler_params=pltpu.CompilerParams(collective_id=0, has_side_effects=True, vmem_limit_bytes=63 * 2**20),
        )(x, gain[None], cos, sin, wq, wk, wv, wo)

    tokens, whole = P(("dp", "sp"), None), P(None, None)
    return jax.shard_map(
        step,
        mesh=mesh,
        in_specs=(tokens, P(None), whole, whole, whole, whole),
        out_specs=tokens,
        check_vma=False,
    )
```

```python
import jax
import jax.numpy as jnp
import numpy as np
from jax import lax
from jax.experimental import pallas as pl
from jax.experimental.pallas import tpu as pltpu
from jax.sharding import PartitionSpec as P

HEAD = 128
THETA = 10000
NEG = -1e30
HIDDEN = 2 * NEG
LOG2E = 1.4426950408889634
E = HEAD**-0.5 * LOG2E
F32, BF16 = jnp.float32, jnp.bfloat16
MESH = pl.DeviceIdType.MESH

OWN = 128
CHIP = 256
D = 4096
G = 4
COLS = G * CHIP
BLOCK = 2 * CHIP
PIECE = 512
STRIP = 512
SUM = HEAD + 8


def _dot(a, b, ca=1, cb=0):
    return lax.dot_general(a, b, (((ca,), (cb,)), ((), ())), preferred_element_type=F32)


def _kernel(x_hbm, gain, freq, wq, wk, wv, wo, y_hbm, w, xs, a, cos, sin, kvs, kv, qs, qr, top, mix, gap, os, orr, acc, out,
            xl_sem, w_sem, wo_sem, xs_sem, xr_sem, kvg_s, kv_r, y_s, z_s, f_s, q_s, q_r, o_s, o_r, out_sem):
    dev = lax.axis_index("sp")
    c = lax.rem(dev, 2)
    chip = lax.div(dev, 2)
    px, py, zh, zl = lax.div(chip, 8), lax.rem(lax.div(chip, 4), 2), lax.rem(lax.div(chip, 2), 2), lax.rem(chip, 2)
    role = px * 2 + zl
    group = py * 2 + zh

    def slot(r, g=group):
        return lax.div(r, 2) * 8 + g * 2 + lax.rem(r, 2)

    def at(r, cc):
        return slot(r) * 2 + cc

    def flip(d):
        dx, dz = (d // 2, d % 2) if isinstance(d, int) else (lax.div(d, 2), lax.rem(d, 2))
        return (px + dx - 2 * px * dx) * 2 + (zl + dz - 2 * zl * dz)

    def send(src, dst, ss, rs, to):
        return pltpu.make_async_remote_copy(src_ref=src, dst_ref=dst, send_sem=ss, recv_sem=rs, device_id={"sp": to}, device_id_type=MESH)

    partner = at(role, 1 - c)
    y_dev = dev + (1 - 2 * py) * 8
    z_dev = dev + (1 - 2 * zh) * 4
    mine = pl.multiple_of(c * OWN, OWN)
    theirs = pl.multiple_of((1 - c) * OWN, OWN)
    cut = pl.multiple_of(c * PIECE, PIECE)

    x_load = pltpu.make_async_copy(x_hbm, xs.at[pl.ds(mine, OWN), :], xl_sem)
    x_load.start()
    wk_load = pltpu.make_async_copy(wk.at[:, pl.ds(cut, PIECE)], w.at[0], w_sem.at[0])
    wv_load = pltpu.make_async_copy(wv.at[:, pl.ds(cut, PIECE)], w.at[1], w_sem.at[1])
    order = (3, 1, 2, 0)

    def q_load(i):
        col = pl.multiple_of((c * 4 + flip(order[i])) * PIECE, PIECE)
        return pltpu.make_async_copy(wq.at[:, pl.ds(col, PIECE)], w.at[2 + i], w_sem.at[2 + i])

    def wo_load(n):
        return pltpu.make_async_copy(wo.at[:, n * PIECE : (n + 1) * PIECE], w.at[(n + 6) % 8], wo_sem.at[n])

    barrier = pltpu.get_barrier_semaphore()

    def greet(to):
        pl.semaphore_signal(barrier, inc=1, device_id={"sp": to}, device_id_type=MESH)

    greet(partner)
    for d in (1, 2, 3):
        greet(at(flip(d), c))
        greet(at(flip(d), 1 - c))
    greet(y_dev)
    greet(z_dev)

    x_load.wait()
    wk_load.start()
    wv_load.start()
    pl.semaphore_wait(barrier, 9)

    x_send = send(xs.at[pl.ds(mine, OWN), :], xs.at[pl.ds(mine, OWN), :], xs_sem, xr_sem, partner)
    x_send.start()

    def norm(first):
        def rows(i, _):
            here = pl.ds(pl.multiple_of(first + i * 16, 16), 16)
            wide = xs[here, :].astype(F32)
            scale = lax.rsqrt(jnp.mean(wide * wide, -1, keepdims=True) + 1e-6)
            a[here, :] = (wide * scale * gain[...].astype(F32)).astype(BF16)
            return 0

        lax.fori_loop(0, OWN // 16, rows, 0, unroll=2)

    place = (chip * CHIP + lax.broadcasted_iota(jnp.int32, (CHIP, HEAD), 0)).astype(F32)
    angle = place * freq[...]
    cos[...] = jnp.cos(angle)
    turn = jnp.sin(angle)
    sin[...] = jnp.where(lax.broadcasted_iota(jnp.int32, (CHIP, HEAD), 1) < HEAD // 2, -turn, turn)

    def turned(h, here):
        h = h.astype(BF16).astype(F32)
        return (h * cos[here, :] + pltpu.roll(h, HEAD // 2, 1) * sin[here, :]).astype(BF16)

    def keys_values(first, n):
        here = pl.ds(first, OWN)
        t = _dot(a[here, :], w[0])
        for j in range(4):
            kvs[j, here, :] = turned(t[:, j * HEAD : (j + 1) * HEAD], here)
        if n == 0:
            wv_load.wait()
        t = _dot(a[here, :], w[1])
        for j in range(4):
            kvs[j, pl.ds(pl.multiple_of(CHIP + first, OWN), HEAD), :] = t[:, j * HEAD : (j + 1) * HEAD].T.astype(BF16)

    norm(mine)
    wk_load.wait()
    for i in range(4):
        q_load(i).start()
    wo_load(0).start()
    wo_load(1).start()
    keys_values(mine, 0)
    send(xs.at[pl.ds(theirs, OWN), :], xs.at[pl.ds(theirs, OWN), :], xs_sem, xr_sem, partner).wait_recv()
    norm(theirs)
    keys_values(theirs, 1)
    wo_load(2).start()
    wo_load(3).start()

    heads = [send(kvs.at[flip(d)], kv.at[chip], kvg_s.at[d - 1], kv_r.at[chip], at(flip(d), c)) for d in (1, 2, 3)]
    for s in heads:
        s.start()
    kv[chip] = kvs[role]

    def along_y(xx):
        return (xx == 0) | (py == 0)

    def along_z(xx):
        return (xx == 0) | (zh == 0) | (py == 0)

    def y_send(s):
        return send(kv.at[s], kv.at[s], y_s.at[s], kv_r.at[s], y_dev)

    def z_send(s):
        return send(kv.at[s], kv.at[s], z_s.at[s], kv_r.at[s], z_dev)

    def arrived(s):
        send(kv.at[s], kv.at[s], y_s.at[s], kv_r.at[s], partner).wait_recv()

    def share(r):
        s, xx = slot(r), lax.div(r, 2)

        @pl.when(along_z(xx))
        def _():
            z_send(s).start()

        @pl.when(along_y(xx))
        def _():
            y_send(s).start()

    share(role)

    mix[...] = jnp.zeros_like(mix)
    top[...] = jnp.full_like(top, NEG)
    gap[...] = lax.rem(lax.broadcasted_iota(jnp.int32, (BLOCK, STRIP), 1), CHIP) - lax.broadcasted_iota(jnp.int32, (BLOCK, STRIP), 0)

    for i in range(4):
        d = order[i]
        q_load(i).wait()
        t = _dot(a[...], w[2 + i])
        dst = qr.at[role] if d == 0 else qs.at[d]
        for g in range(G):
            dst[g * CHIP : (g + 1) * CHIP, :] = turned(t[:, g * HEAD : (g + 1) * HEAD], slice(None))
        wo_load(4 + i).start()
        if i == 2:
            for s in heads:
                s.wait_send()
            for n in order[:3]:
                send(qs.at[n], qr.at[role], q_s.at[n - 1], q_r.at[role], at(flip(n), c)).start()

    def sharing(n, _):
        d = jnp.where(px == 0, n, jnp.where(n == 3, 1, n + 1))
        r = flip(d)
        arrived(slot(r))
        share(r)
        return 0

    lax.fori_loop(1, 4, sharing, 0)

    ones = jnp.ones((8, BLOCK), BF16)

    def item(q, m, masked):
        halves = (kv[2 * m], kv[2 * m + 1])
        keys = jnp.concatenate([h[:CHIP] for h in halves], axis=0)
        values = jnp.concatenate([h[i : i + HEAD] for h in halves for i in (CHIP, CHIP + HEAD)], axis=1)
        values = jnp.concatenate([values, ones], axis=0)
        strips = [(n * STRIP, n // 2, n % 2 * STRIP) for n in range(2 * COLS // STRIP)]
        seen = [CHIP if masked and half == 0 else BLOCK for _, half, _ in strips]
        scores = [_dot(keys[:n], qr[q * 2 + half, i : i + STRIP, :], 1, 1) for (_, half, i), n in zip(strips, seen)]
        weights, keeps = [], []
        for (col, half, _), n, v in zip(strips, seen, scores):
            if masked:
                v = jnp.where(gap[:n, :] >= -half * CHIP, v, HIDDEN)
            old = top[q, 0:1, col : col + STRIP]
            new = jnp.maximum(old, v.max(axis=0, keepdims=True))
            top[q, 0:1, col : col + STRIP] = new
            weights.append(jnp.exp2((v - new) * E).astype(BF16))
            keeps.append(jnp.exp2((old - new) * E))
        for (col, _, _), n, v, keep in zip(strips, seen, weights, keeps):
            mix[q, :, col : col + STRIP] = mix[q, :, col : col + STRIP] * keep + _dot(values[:, :n], v)

    y_group, z_group, far_group = (1 - py) * 2 + zh, py * 2 + 1 - zh, (1 - py) * 2 + 1 - zh

    def take(g, xx):
        sent = {"y": (xx == 0) | (py == 1), "z": (xx == 0) | (zh == 1) | (py == 0), "far": (xx == 0) | (py == 1)}[g]
        number = {"y": y_group, "z": z_group, "far": far_group}[g]

        @pl.when(sent)
        def _():
            for n in range(2):
                s = slot(xx * 2 + n, number)
                arrived(s)
                if g == "z":

                    @pl.when(along_y(xx))
                    def _():
                        send(kv.at[s], kv.at[s], f_s.at[s], kv_r.at[s], y_dev).start()

    def q_arrived(r):
        send(qs.at[1], qr.at[r], q_s.at[0], q_r.at[r], partner).wait_recv()

    def full(q, m):
        @pl.when(m < q * 4 + group)
        def _():
            item(q, m, False)

    def phase(n, _):
        q = jnp.where(n == 0, px, 1 - px)

        @pl.when(n == 0)
        def _():
            q_arrived(flip(1))

        @pl.when(n == 1)
        def _():
            q_arrived(flip(2))
            q_arrived(flip(3))

        item(q, q * 4 + group, True)

        def block(i, _):
            @pl.when((n == 0) & (i == 1))
            def _():
                take("y", 0)

            @pl.when((n == 0) & (i == 2))
            def _():
                take("z", 0)

            @pl.when((n == 0) & (i == 3))
            def _():
                take("y", 1)

            m = jnp.where(i == 0, group, jnp.where(i == 1, y_group, jnp.where(i == 2, z_group, 4 + y_group)))
            full(q, m)
            return 0

        lax.fori_loop(0, 4, block, 0)
        return 0

    lax.fori_loop(0, 2, phase, 0)

    def finish(q):
        total = mix[q, HEAD : HEAD + 1, :]
        o = mix[q, :HEAD, :] * (1 / total)
        for n in range(2):
            r = q * 2 + n
            for g in range(G):
                for h in range(2):
                    first = n * COLS + g * CHIP + h * OWN
                    os[r, h, :, g * HEAD : (g + 1) * HEAD] = o[:, first : first + OWN].T.astype(BF16)
            for h in range(2):
                to = at(r, h)

                @pl.when(to != dev)
                def _():
                    send(os.at[r, h], orr.at[c * 4 + role], o_s.at[r, h], o_r.at[c * 4 + role], to).start()

                @pl.when(to == dev)
                def _():
                    orr[c * 4 + role] = os[r, h]

    def last(i, _):
        @pl.when(i == 0)
        def _():
            take("z", 1)
            take("far", 0)

        @pl.when(i == 3)
        def _():
            take("far", 1)

        full(jnp.where(i == 0, 0, 1), jnp.where(i < 2, far_group, jnp.where(i == 2, 4 + z_group, 4 + far_group)))

        @pl.when(i == 0)
        def _():
            finish(0)

        @pl.when(i == 3)
        def _():
            finish(1)

        return 0

    lax.fori_loop(0, 4, last, 0)

    for n in range(8):
        wo_load(n).wait()

    def project(d, _):
        r = flip(d)
        for cc in range(2):
            j = cc * 4 + r

            @pl.when(at(r, cc) != dev)
            def _():
                send(os.at[0, 0], orr.at[j], o_s.at[0, 0], o_r.at[j], partner).wait_recv()

        for n in range(8):
            here = slice(n * PIECE, (n + 1) * PIECE)
            t = acc[:, here]
            for cc in range(2):
                j = cc * 4 + r
                t = t + _dot(orr[j], w[(n + 6) % 8, pl.ds(pl.multiple_of(j * PIECE, PIECE), PIECE), :])
            acc[:, here] = t
        return 0

    acc[...] = xs[pl.ds(mine, OWN), :].astype(F32)
    lax.fori_loop(0, 4, project, 0)
    out[...] = acc[...].astype(BF16)
    store = pltpu.make_async_copy(out, y_hbm, out_sem)
    store.start()

    x_send.wait_send()
    for d in (1, 2, 3):
        send(qs.at[d], qr.at[role], q_s.at[d - 1], q_r.at[role], partner).wait_send()

    def left(r, _):
        s, xx = slot(r), lax.div(r, 2)

        @pl.when(along_z(xx))
        def _():
            z_send(s).wait_send()

        @pl.when(along_y(xx))
        def _():
            y_send(s).wait_send()

        came = slot(r, z_group)

        @pl.when(((xx == 0) | (zh == 1) | (py == 0)) & along_y(xx))
        def _():
            send(kv.at[came], kv.at[came], f_s.at[came], kv_r.at[came], y_dev).wait_send()

        for h in range(2):

            @pl.when(at(r, h) != dev)
            def _():
                send(os.at[r, h], orr.at[0], o_s.at[r, h], o_r.at[0], partner).wait_send()

        return 0

    lax.fori_loop(0, 4, left, 0)
    store.wait()


def solution(mesh):
    def step(x, gain, wq, wk, wv, wo):
        half = HEAD // 2
        freq = (THETA ** (-np.arange(half, dtype=np.float32) / half)).astype(np.float32)
        freq = jnp.asarray(np.tile(freq, 2)[None])
        vmem, hbm = pl.BlockSpec(memory_space=pltpu.VMEM), pl.BlockSpec(memory_space=pl.ANY)
        dma = pltpu.SemaphoreType.DMA
        return pl.pallas_call(
            _kernel,
            out_shape=jax.ShapeDtypeStruct((OWN, D), BF16),
            in_specs=[hbm, vmem, vmem, hbm, hbm, hbm, hbm],
            out_specs=hbm,
            scratch_shapes=[
                pltpu.VMEM((8, D, PIECE), BF16),
                pltpu.VMEM((CHIP, D), BF16),
                pltpu.VMEM((CHIP, D), BF16),
                pltpu.VMEM((CHIP, HEAD), F32),
                pltpu.VMEM((CHIP, HEAD), F32),
                pltpu.VMEM((4, 2 * CHIP, HEAD), BF16),
                pltpu.VMEM((16, 2 * CHIP, HEAD), BF16),
                pltpu.VMEM((4, COLS, HEAD), BF16),
                pltpu.VMEM((4, COLS, HEAD), BF16),
                pltpu.VMEM((2, 8, 2 * COLS), F32),
                pltpu.VMEM((2, SUM, 2 * COLS), F32),
                pltpu.VMEM((BLOCK, STRIP), jnp.int32),
                pltpu.VMEM((4, 2, OWN, PIECE), BF16),
                pltpu.VMEM((8, OWN, PIECE), BF16),
                pltpu.VMEM((OWN, D), F32),
                pltpu.VMEM((OWN, D), BF16),
                dma, dma((6,)), dma((8,)), dma, dma, dma((3,)), dma((16,)), dma((16,)), dma((16,)), dma((16,)), dma((3,)), dma((4,)),
                dma((4, 2)), dma((8,)), dma,
            ],
            compiler_params=pltpu.CompilerParams(collective_id=0, has_side_effects=True, vmem_limit_bytes=63 * 2**20),
        )(x, gain[None], freq, wq, wk, wv, wo)

    tokens, whole = P(("dp", "sp"), None), P(None, None)
    return jax.shard_map(
        step,
        mesh=mesh,
        in_specs=(tokens, P(None), whole, whole, whole, whole),
        out_specs=tokens,
        check_vma=False,
    )
```

```python
import jax
import jax.numpy as jnp
import numpy as np
from jax import lax
from jax.experimental import pallas as pl
from jax.experimental.pallas import tpu as pltpu
from jax.sharding import PartitionSpec as P

HEAD = 128
THETA = 10000
NEG = -1e30
HIDDEN = 2 * NEG
LOG2E = 1.4426950408889634
E = HEAD**-0.5 * LOG2E
F32, BF16 = jnp.float32, jnp.bfloat16
MESH = pl.DeviceIdType.MESH

OWN = 128
CHIP = 256
D = 4096
G = 4
COLS = G * CHIP
BLOCK = 2 * CHIP
PIECE = 512
STRIP = 512
SUM = HEAD + 8


def _dot(a, b, ca=1, cb=0):
    return lax.dot_general(a, b, (((ca,), (cb,)), ((), ())), preferred_element_type=F32)


def _kernel(x_hbm, gain, freq, wq, wk, wv, wo, y_hbm, w, xs, a, cos, sin, kvs, kv, qs, qr, top, mix, gap, os, orr, acc, out,
            xl_sem, w_sem, wo_sem, xs_sem, xr_sem, kvg_s, kv_r, y_s, z_s, f_s, q_s, q_r, o_s, o_r, out_sem):
    dev = lax.axis_index("sp")
    c = lax.rem(dev, 2)
    chip = lax.div(dev, 2)
    px, py, zh, zl = lax.div(chip, 8), lax.rem(lax.div(chip, 4), 2), lax.rem(lax.div(chip, 2), 2), lax.rem(chip, 2)
    role = px * 2 + zl
    group = py * 2 + zh

    def slot(r, g=group):
        return lax.div(r, 2) * 8 + g * 2 + lax.rem(r, 2)

    def at(r, cc):
        return slot(r) * 2 + cc

    def flip(d):
        dx, dz = (d // 2, d % 2) if isinstance(d, int) else (lax.div(d, 2), lax.rem(d, 2))
        return (px + dx - 2 * px * dx) * 2 + (zl + dz - 2 * zl * dz)

    def send(src, dst, ss, rs, to):
        return pltpu.make_async_remote_copy(src_ref=src, dst_ref=dst, send_sem=ss, recv_sem=rs, device_id={"sp": to}, device_id_type=MESH)

    partner = at(role, 1 - c)
    y_dev = dev + (1 - 2 * py) * 8
    z_dev = dev + (1 - 2 * zh) * 4
    mine = pl.multiple_of(c * OWN, OWN)
    theirs = pl.multiple_of((1 - c) * OWN, OWN)
    cut = pl.multiple_of(c * PIECE, PIECE)

    x_load = pltpu.make_async_copy(x_hbm, xs.at[pl.ds(mine, OWN), :], xl_sem)
    x_load.start()
    wk_load = pltpu.make_async_copy(wk.at[:, pl.ds(cut, PIECE)], w.at[0], w_sem.at[0])
    wv_load = pltpu.make_async_copy(wv.at[:, pl.ds(cut, PIECE)], w.at[1], w_sem.at[1])
    order = (2, 1, 3, 0)

    def q_load(i):
        col = pl.multiple_of((c * 4 + flip(order[i])) * PIECE, PIECE)
        return pltpu.make_async_copy(wq.at[:, pl.ds(col, PIECE)], w.at[2 + i], w_sem.at[2 + i])

    def wo_load(n):
        return pltpu.make_async_copy(wo.at[:, n * PIECE : (n + 1) * PIECE], w.at[(n + 6) % 8], wo_sem.at[n])

    barrier = pltpu.get_barrier_semaphore()

    def greet(to):
        pl.semaphore_signal(barrier, inc=1, device_id={"sp": to}, device_id_type=MESH)

    greet(partner)
    for d in (1, 2, 3):
        greet(at(flip(d), c))
        greet(at(flip(d), 1 - c))
    greet(y_dev)
    greet(z_dev)

    x_load.wait()
    wk_load.start()
    wv_load.start()
    pl.semaphore_wait(barrier, 9)

    x_send = send(xs.at[pl.ds(mine, OWN), :], xs.at[pl.ds(mine, OWN), :], xs_sem, xr_sem, partner)
    x_send.start()

    def norm(first):
        def rows(i, _):
            here = pl.ds(pl.multiple_of(first + i * 16, 16), 16)
            wide = xs[here, :].astype(F32)
            scale = lax.rsqrt(jnp.mean(wide * wide, -1, keepdims=True) + 1e-6)
            a[here, :] = (wide * scale * gain[...].astype(F32).reshape(1, D)).astype(BF16)
            return 0

        lax.fori_loop(0, OWN // 16, rows, 0, unroll=2)

    place = (chip * CHIP + lax.broadcasted_iota(jnp.int32, (CHIP, HEAD), 0)).astype(F32)
    angle = place * freq[...]
    cos[...] = jnp.cos(angle)
    turn = jnp.sin(angle)
    sin[...] = jnp.where(lax.broadcasted_iota(jnp.int32, (CHIP, HEAD), 1) < HEAD // 2, -turn, turn)

    def turned(h, here):
        h = h.astype(BF16).astype(F32)
        return (h * cos[here, :] + pltpu.roll(h, HEAD // 2, 1) * sin[here, :]).astype(BF16)

    def keys_values(first, n):
        here = pl.ds(first, OWN)
        t = _dot(a[here, :], w[0])
        for j in range(4):
            kvs[j, here, :] = turned(t[:, j * HEAD : (j + 1) * HEAD], here)
        if n == 0:
            wv_load.wait()
        t = _dot(a[here, :], w[1])
        for j in range(4):
            kvs[j, pl.ds(pl.multiple_of(CHIP + first, OWN), HEAD), :] = t[:, j * HEAD : (j + 1) * HEAD].T.astype(BF16)

    norm(mine)
    wk_load.wait()
    for i in range(4):
        q_load(i).start()
    wo_load(0).start()
    wo_load(1).start()
    keys_values(mine, 0)
    send(xs.at[pl.ds(theirs, OWN), :], xs.at[pl.ds(theirs, OWN), :], xs_sem, xr_sem, partner).wait_recv()
    norm(theirs)
    keys_values(theirs, 1)
    wo_load(2).start()
    wo_load(3).start()

    heads = [send(kvs.at[flip(d)], kv.at[chip], kvg_s.at[d - 1], kv_r.at[chip], at(flip(d), c)) for d in (1, 2, 3)]
    for s in heads:
        s.start()
    kv[chip] = kvs[role]

    def along_y(xx):
        return (xx == 0) | (py == 0)

    def along_z(xx):
        return (xx == 0) | (zh == 0) | (py == 0)

    def y_send(s):
        return send(kv.at[s], kv.at[s], y_s.at[s], kv_r.at[s], y_dev)

    def z_send(s):
        return send(kv.at[s], kv.at[s], z_s.at[s], kv_r.at[s], z_dev)

    def arrived(s):
        send(kv.at[s], kv.at[s], y_s.at[s], kv_r.at[s], partner).wait_recv()

    def share_z(r, xx):
        @pl.when((lax.div(r, 2) == xx) & along_z(xx))
        def _():
            z_send(slot(r)).start()

    def share(r):
        share_z(r, 0)

        @pl.when(along_y(lax.div(r, 2)))
        def _():
            y_send(slot(r)).start()

    share(role)

    mix[...] = jnp.zeros_like(mix)
    top[...] = jnp.full_like(top, NEG)
    gap[...] = lax.rem(lax.broadcasted_iota(jnp.int32, (BLOCK, STRIP), 1), CHIP) - lax.broadcasted_iota(jnp.int32, (BLOCK, STRIP), 0)

    for i in range(4):
        d = order[i]
        q_load(i).wait()
        t = _dot(a[...], w[2 + i])
        dst = qr.at[role] if d == 0 else qs.at[d]
        for g in range(G):
            dst[g * CHIP : (g + 1) * CHIP, :] = turned(t[:, g * HEAD : (g + 1) * HEAD], slice(None))
        wo_load(4 + i).start()
        if i == 2:
            for s in heads:
                s.wait_send()
            for n in order[:3]:
                send(qs.at[n], qr.at[role], q_s.at[n - 1], q_r.at[role], at(flip(n), c)).start()

    def sharing(n, _):
        d = jnp.where(px == 0, n, jnp.where(n == 3, 1, n + 1))
        r = flip(d)
        arrived(slot(r))
        share(r)
        return 0

    lax.fori_loop(1, 4, sharing, 0)

    ones = jnp.ones((8, BLOCK), BF16)

    def item(r, m, masked):
        halves = (kv[2 * m], kv[2 * m + 1])
        keys = jnp.concatenate([h[:CHIP] for h in halves], axis=0)
        values = jnp.concatenate([h[i : i + HEAD] for h in halves for i in (CHIP, CHIP + HEAD)], axis=1)
        values = jnp.concatenate([values, ones], axis=0)
        strips = range(0, COLS, STRIP)
        scores = [_dot(keys, qr[r, i : i + STRIP, :], 1, 1) for i in strips]
        weights, keeps = [], []
        for i, v in zip(strips, scores):
            if masked:
                v = jnp.where(gap[...] >= -CHIP * lax.rem(r, 2), v, HIDDEN)
            old = top[r, 0:1, i : i + STRIP]
            new = jnp.maximum(old, v.max(axis=0, keepdims=True))
            top[r, 0:1, i : i + STRIP] = new
            weights.append(jnp.exp2((v - new) * E).astype(BF16))
            keeps.append(jnp.exp2((old - new) * E))
        for i, v, keep in zip(strips, weights, keeps):
            mix[r, :, i : i + STRIP] = mix[r, :, i : i + STRIP] * keep + _dot(values, v)

    y_group, z_group, far_group = (1 - py) * 2 + zh, py * 2 + 1 - zh, (1 - py) * 2 + 1 - zh

    def take(g, xx):
        sent = {"y": (xx == 0) | (py == 1), "z": (xx == 0) | (zh == 1) | (py == 0), "far": (xx == 0) | (py == 1)}[g]
        number = {"y": y_group, "z": z_group, "far": far_group}[g]

        @pl.when(sent)
        def _():
            for n in range(2):
                s = slot(xx * 2 + n, number)
                arrived(s)
                if g == "z":

                    @pl.when(along_y(xx))
                    def _():
                        send(kv.at[s], kv.at[s], f_s.at[s], kv_r.at[s], y_dev).start()

    def q_arrived(r):
        send(qs.at[1], qr.at[r], q_s.at[0], q_r.at[r], partner).wait_recv()

    def full(n, task):
        def one(i, _):
            r, m = task(i)

            @pl.when(m < lax.div(r, 2) * 4 + group)
            def _():
                item(r, m, False)

            return 0

        lax.fori_loop(0, n, one, 0)

    def pick(i, *choices):
        got = choices[-1]
        for n in range(len(choices) - 2, -1, -1):
            got = jnp.where(i == n, choices[n], got)
        return got

    def diagonal(r):
        item(r, lax.div(r, 2) * 4 + group, True)

    def finish(r):
        o = mix[r, :HEAD, :] * (1 / mix[r, HEAD : HEAD + 1, :])
        for g in range(G):
            for h in range(2):
                first = g * CHIP + h * OWN
                os[r, h, :, g * HEAD : (g + 1) * HEAD] = o[:, first : first + OWN].T.astype(BF16)
        for h in range(2):
            to = at(r, h)

            @pl.when(to != dev)
            def _():
                send(os.at[r, h], orr.at[c * 4 + role], o_s.at[r, h], o_r.at[c * 4 + role], to).start()

            @pl.when(to == dev)
            def _():
                orr[c * 4 + role] = os[r, h]

    beside = flip(2)
    diagonal(role)
    take("y", 0)
    take("y", 1)
    full(3, lambda i: (role, pick(i, group, y_group, 4 + y_group)))
    for d in range(4):
        share_z(flip(d), 1)
    q_arrived(beside)
    diagonal(beside)
    full(3, lambda i: (beside, pick(i, group, y_group, 4 + y_group)))
    take("z", 0)
    full(2, lambda i: (pick(i, role, beside), z_group))
    take("far", 0)
    full(2, lambda i: (pick(i, role, beside), far_group))
    q_arrived(flip(1))
    q_arrived(flip(3))

    def others(n, _):
        r = flip(2 * n + 1)
        diagonal(r)
        full(5, lambda i: (r, pick(i, group, y_group, 4 + y_group, z_group, far_group)))

        @pl.when(n == 0)
        def _():
            take("z", 1)

        return 0

    lax.fori_loop(0, 2, others, 0)

    def ending(n, _):
        lax.fori_loop(0, 2, lambda i, _: (finish(n * 2 + i), 0)[1], 0)

        @pl.when(n == 0)
        def _():
            full(2, lambda i: (2 + i, 4 + z_group))
            take("far", 1)
            full(2, lambda i: (2 + i, 4 + far_group))

        return 0

    lax.fori_loop(0, 2, ending, 0)

    for n in range(8):
        wo_load(n).wait()

    def project(d, _):
        r = flip(d)
        for cc in range(2):
            j = cc * 4 + r

            @pl.when(at(r, cc) != dev)
            def _():
                send(os.at[0, 0], orr.at[j], o_s.at[0, 0], o_r.at[j], partner).wait_recv()

        for n in range(8):
            here = slice(n * PIECE, (n + 1) * PIECE)
            t = acc[:, here]
            for cc in range(2):
                j = cc * 4 + r
                t = t + _dot(orr[j], w[(n + 6) % 8, pl.ds(pl.multiple_of(j * PIECE, PIECE), PIECE), :])
            acc[:, here] = t
        return 0

    acc[...] = xs[pl.ds(mine, OWN), :].astype(F32)
    lax.fori_loop(0, 4, project, 0)
    out[...] = acc[...].astype(BF16)
    store = pltpu.make_async_copy(out, y_hbm, out_sem)
    store.start()

    x_send.wait_send()
    for d in (1, 2, 3):
        send(qs.at[d], qr.at[role], q_s.at[d - 1], q_r.at[role], partner).wait_send()

    def left(r, _):
        s, xx = slot(r), lax.div(r, 2)

        @pl.when(along_z(xx))
        def _():
            z_send(s).wait_send()

        @pl.when(along_y(xx))
        def _():
            y_send(s).wait_send()

        came = slot(r, z_group)

        @pl.when(((xx == 0) | (zh == 1) | (py == 0)) & along_y(xx))
        def _():
            send(kv.at[came], kv.at[came], f_s.at[came], kv_r.at[came], y_dev).wait_send()

        for h in range(2):

            @pl.when(at(r, h) != dev)
            def _():
                send(os.at[r, h], orr.at[0], o_s.at[r, h], o_r.at[0], partner).wait_send()

        return 0

    lax.fori_loop(0, 4, left, 0)
    store.wait()


def solution(mesh):
    def step(x, gain, wq, wk, wv, wo):
        half = HEAD // 2
        freq = (THETA ** (-np.arange(half, dtype=np.float32) / half)).astype(np.float32)
        freq = jnp.asarray(np.tile(freq, 2)[None])
        vmem, hbm = pl.BlockSpec(memory_space=pltpu.VMEM), pl.BlockSpec(memory_space=pl.ANY)
        dma = pltpu.SemaphoreType.DMA
        return pl.pallas_call(
            _kernel,
            out_shape=jax.ShapeDtypeStruct((OWN, D), BF16),
            in_specs=[hbm, vmem, vmem, hbm, hbm, hbm, hbm],
            out_specs=hbm,
            scratch_shapes=[
                pltpu.VMEM((8, D, PIECE), BF16),
                pltpu.VMEM((CHIP, D), BF16),
                pltpu.VMEM((CHIP, D), BF16),
                pltpu.VMEM((CHIP, HEAD), F32),
                pltpu.VMEM((CHIP, HEAD), F32),
                pltpu.VMEM((4, 2 * CHIP, HEAD), BF16),
                pltpu.VMEM((16, 2 * CHIP, HEAD), BF16),
                pltpu.VMEM((4, COLS, HEAD), BF16),
                pltpu.VMEM((4, COLS, HEAD), BF16),
                pltpu.VMEM((4, 8, COLS), F32),
                pltpu.VMEM((4, SUM, COLS), F32),
                pltpu.VMEM((BLOCK, STRIP), jnp.int32),
                pltpu.VMEM((4, 2, OWN, PIECE), BF16),
                pltpu.VMEM((8, OWN, PIECE), BF16),
                pltpu.VMEM((OWN, D), F32),
                pltpu.VMEM((OWN, D), BF16),
                dma, dma((6,)), dma((8,)), dma, dma, dma((3,)), dma((16,)), dma((16,)), dma((16,)), dma((16,)), dma((3,)), dma((4,)),
                dma((4, 2)), dma((8,)), dma,
            ],
            compiler_params=pltpu.CompilerParams(collective_id=0, has_side_effects=True, vmem_limit_bytes=63 * 2**20),
        )(x, gain, freq, wq, wk, wv, wo)

    tokens, whole = P(("dp", "sp"), None), P(None, None)
    return jax.shard_map(
        step,
        mesh=mesh,
        in_specs=(tokens, P(None), whole, whole, whole, whole),
        out_specs=tokens,
        check_vma=False,
    )
```

```python
import jax
import jax.numpy as jnp
import numpy as np
from jax import lax
from jax.experimental import pallas as pl
from jax.experimental.pallas import tpu as pltpu
from jax.sharding import PartitionSpec as P

HEAD = 128
THETA = 10000
NEG = -1e30
HIDDEN = 2 * NEG
LOG2E = 1.4426950408889634
E = HEAD**-0.5 * LOG2E
F32, BF16 = jnp.float32, jnp.bfloat16
MESH = pl.DeviceIdType.MESH

OWN = 128
CHIP = 256
D = 4096
G = 4
COLS = G * CHIP
BLOCK = 2 * CHIP
PIECE = 512
STRIP = 512
SUM = HEAD + 8


def _dot(a, b, ca=1, cb=0):
    return lax.dot_general(a, b, (((ca,), (cb,)), ((), ())), preferred_element_type=F32)


def _kernel(x_hbm, gain, freq, wq, wk, wv, wo, y_hbm, w, xs, a, cos, sin, kvs, kv, qs, qr, top, mix, gap, os, orr, acc, out,
            xl_sem, w_sem, wo_sem, xs_sem, xr_sem, kvg_s, kvg_r, kv_r, y_s, z_s, f_s, q_s, q_r, o_s, o_r, out_sem):
    dev = lax.axis_index("sp")
    c = lax.rem(dev, 2)
    chip = lax.div(dev, 2)
    px, py, zh, zl = lax.div(chip, 8), lax.rem(lax.div(chip, 4), 2), lax.rem(lax.div(chip, 2), 2), lax.rem(chip, 2)
    role = px * 2 + zl
    group = py * 2 + zh

    def slot(r, g=group):
        return lax.div(r, 2) * 8 + g * 2 + lax.rem(r, 2)

    def at(r, cc):
        return slot(r) * 2 + cc

    def flip(d):
        dx, dz = (d // 2, d % 2) if isinstance(d, int) else (lax.div(d, 2), lax.rem(d, 2))
        return (px + dx - 2 * px * dx) * 2 + (zl + dz - 2 * zl * dz)

    def send(src, dst, ss, rs, to):
        return pltpu.make_async_remote_copy(src_ref=src, dst_ref=dst, send_sem=ss, recv_sem=rs, device_id={"sp": to}, device_id_type=MESH)

    partner = at(role, 1 - c)
    y_dev = dev + (1 - 2 * py) * 8
    z_dev = dev + (1 - 2 * zh) * 4
    mine = pl.multiple_of(c * OWN, OWN)
    theirs = pl.multiple_of((1 - c) * OWN, OWN)
    cut = pl.multiple_of(c * PIECE, PIECE)

    x_load = pltpu.make_async_copy(x_hbm, xs.at[pl.ds(mine, OWN), :], xl_sem)
    x_load.start()
    wk_load = pltpu.make_async_copy(wk.at[:, pl.ds(cut, PIECE)], w.at[0], w_sem.at[0])
    wv_load = pltpu.make_async_copy(wv.at[:, pl.ds(cut, PIECE)], w.at[1], w_sem.at[1])
    order = (2, 1, 3, 0)

    def q_load(i):
        col = pl.multiple_of((c * 4 + flip(order[i])) * PIECE, PIECE)
        return pltpu.make_async_copy(wq.at[:, pl.ds(col, PIECE)], w.at[2 + i], w_sem.at[2 + i])

    def wo_load(n):
        return pltpu.make_async_copy(wo.at[:, n * PIECE : (n + 1) * PIECE], w.at[(n + 6) % 8], wo_sem.at[n])

    barrier = pltpu.get_barrier_semaphore()

    def greet(to):
        pl.semaphore_signal(barrier, inc=1, device_id={"sp": to}, device_id_type=MESH)

    greet(partner)
    for d in (1, 2, 3):
        greet(at(flip(d), c))
        greet(at(flip(d), 1 - c))
    greet(y_dev)
    greet(z_dev)

    place = (chip * CHIP + lax.broadcasted_iota(jnp.int32, (CHIP, HEAD), 0)).astype(F32)
    angle = place * freq[...]
    cos[...] = jnp.cos(angle)
    turn = jnp.sin(angle)
    sin[...] = jnp.where(lax.broadcasted_iota(jnp.int32, (CHIP, HEAD), 1) < HEAD // 2, -turn, turn)

    x_load.wait()
    wk_load.start()
    wv_load.start()
    pl.semaphore_wait(barrier, 9)

    x_send = send(xs.at[pl.ds(mine, OWN), :], xs.at[pl.ds(mine, OWN), :], xs_sem, xr_sem, partner)
    x_send.start()

    def norm(first):
        def rows(i, _):
            here = pl.ds(pl.multiple_of(first + i * 16, 16), 16)
            wide = xs[here, :].astype(F32)
            scale = lax.rsqrt(jnp.mean(wide * wide, -1, keepdims=True) + 1e-6)
            a[here, :] = (wide * scale * gain[...].astype(F32).reshape(1, D)).astype(BF16)
            return 0

        lax.fori_loop(0, OWN // 16, rows, 0, unroll=2)

    def turned(h, here):
        h = h.astype(BF16).astype(F32)
        return (h * cos[here, :] + pltpu.roll(h, HEAD // 2, 1) * sin[here, :]).astype(BF16)

    def half(d, n):
        return send(kvs.at[flip(d), n], kv.at[chip, n], kvg_s.at[d - 1, n], kvg_r.at[role, n], at(flip(d), c))

    def keys_values(first, n, wait):
        here = pl.ds(first, OWN)
        t = _dot(a[here, :], w[0])
        for j in range(4):
            kvs[j, n, :OWN, :] = turned(t[:, j * HEAD : (j + 1) * HEAD], here)
        if wait:
            wv_load.wait()
        t = _dot(a[here, :], w[1])
        for j in range(4):
            kvs[j, n, OWN:, :] = t[:, j * HEAD : (j + 1) * HEAD].T.astype(BF16)
        for d in (1, 2, 3):
            half(d, n).start()

    norm(mine)
    wk_load.wait()
    for i in range(4):
        q_load(i).start()
    wo_load(0).start()
    wo_load(1).start()
    keys_values(mine, c, True)
    send(xs.at[pl.ds(theirs, OWN), :], xs.at[pl.ds(theirs, OWN), :], xs_sem, xr_sem, partner).wait_recv()
    norm(theirs)
    keys_values(theirs, 1 - c, False)
    wo_load(2).start()
    wo_load(3).start()

    kv[chip] = kvs[role]

    def along_y(xx):
        return (xx == 0) | (py == 0)

    def along_z(xx):
        return (xx == 0) | (zh == 0) | (py == 0)

    def y_send(s):
        return send(kv.at[s], kv.at[s], y_s.at[s], kv_r.at[s], y_dev)

    def z_send(s):
        return send(kv.at[s], kv.at[s], z_s.at[s], kv_r.at[s], z_dev)

    def arrived(s):
        send(kv.at[s], kv.at[s], y_s.at[s], kv_r.at[s], partner).wait_recv()

    def half_arrived(r, n):
        send(kvs.at[0, 0], kv.at[slot(r), n], kvg_s.at[0, 0], kvg_r.at[r, n], partner).wait_recv()

    def share_z(r, xx):
        @pl.when((lax.div(r, 2) == xx) & along_z(xx))
        def _():
            z_send(slot(r)).start()

    def share(r):
        share_z(r, 0)

        @pl.when(along_y(lax.div(r, 2)))
        def _():
            y_send(slot(r)).start()

    share(role)

    mix[...] = jnp.zeros_like(mix)
    top[...] = jnp.full_like(top, NEG)
    gap[...] = lax.rem(lax.broadcasted_iota(jnp.int32, (BLOCK, STRIP), 1), CHIP) - lax.broadcasted_iota(jnp.int32, (BLOCK, STRIP), 0)

    for i in range(4):
        d = order[i]
        q_load(i).wait()
        t = _dot(a[...], w[2 + i])
        dst = qr.at[role] if d == 0 else qs.at[d]
        for g in range(G):
            dst[g * CHIP : (g + 1) * CHIP, :] = turned(t[:, g * HEAD : (g + 1) * HEAD], slice(None))
        wo_load(4 + i).start()
        if i == 2:
            for n in range(2):
                for d in (1, 2, 3):
                    half(d, n).wait_send()
            for n in order[:3]:
                send(qs.at[n], qr.at[role], q_s.at[n - 1], q_r.at[role], at(flip(n), c)).start()
        for n in ((), (), (1, 2), (3,))[i]:
            for h in range(2):
                half_arrived(flip(n), h)
            share(flip(n))

    ones = jnp.ones((8, BLOCK), BF16)

    def item(r, m, masked):
        halves = [kv[2 * m + i, n] for i in range(2) for n in range(2)]
        keys = jnp.concatenate([h[:OWN] for h in halves], axis=0)
        values = jnp.concatenate([h[OWN:] for h in halves], axis=1)
        values = jnp.concatenate([values, ones], axis=0)
        strips = range(0, COLS, STRIP)
        scores = [_dot(keys, qr[r, i : i + STRIP, :], 1, 1) for i in strips]
        weights, keeps = [], []
        for i, v in zip(strips, scores):
            if masked:
                v = jnp.where(gap[...] >= -CHIP * lax.rem(r, 2), v, HIDDEN)
            old = top[r, 0:1, i : i + STRIP]
            new = jnp.maximum(old, v.max(axis=0, keepdims=True))
            top[r, 0:1, i : i + STRIP] = new
            weights.append(jnp.exp2((v - new) * E).astype(BF16))
            keeps.append(jnp.exp2((old - new) * E))
        for i, v, keep in zip(strips, weights, keeps):
            mix[r, :, i : i + STRIP] = mix[r, :, i : i + STRIP] * keep + _dot(values, v)

    y_group, z_group, far_group = (1 - py) * 2 + zh, py * 2 + 1 - zh, (1 - py) * 2 + 1 - zh

    def take(g, xx):
        sent = {"y": (xx == 0) | (py == 1), "z": (xx == 0) | (zh == 1) | (py == 0), "far": (xx == 0) | (py == 1)}[g]
        number = {"y": y_group, "z": z_group, "far": far_group}[g]

        @pl.when(sent)
        def _():
            for n in range(2):
                s = slot(xx * 2 + n, number)
                arrived(s)
                if g == "z":

                    @pl.when(along_y(xx))
                    def _():
                        send(kv.at[s], kv.at[s], f_s.at[s], kv_r.at[s], y_dev).start()

    def q_arrived(r):
        send(qs.at[1], qr.at[r], q_s.at[0], q_r.at[r], partner).wait_recv()

    def full(n, task):
        def one(i, _):
            r, m = task(i)

            @pl.when(m < lax.div(r, 2) * 4 + group)
            def _():
                item(r, m, False)

            return 0

        lax.fori_loop(0, n, one, 0)

    def pick(i, *choices):
        got = choices[-1]
        for n in range(len(choices) - 2, -1, -1):
            got = jnp.where(i == n, choices[n], got)
        return got

    def diagonal(r):
        item(r, lax.div(r, 2) * 4 + group, True)

    def finish(r):
        o = mix[r, :HEAD, :] * (1 / mix[r, HEAD : HEAD + 1, :])
        for g in range(G):
            for h in range(2):
                first = g * CHIP + h * OWN
                os[r, h, :, g * HEAD : (g + 1) * HEAD] = o[:, first : first + OWN].T.astype(BF16)
        for h in range(2):
            to = at(r, h)

            @pl.when(to != dev)
            def _():
                send(os.at[r, h], orr.at[c * 4 + role], o_s.at[r, h], o_r.at[c * 4 + role], to).start()

            @pl.when(to == dev)
            def _():
                orr[c * 4 + role] = os[r, h]

    beside = flip(2)
    diagonal(role)
    for d in range(4):
        share_z(flip(d), 1)
    full(1, lambda i: (role, group))

    def beyond(i, _):
        xx = jnp.where(i == 0, px, 1 - px)
        take("y", xx)
        full(1, lambda i: (role, 4 * xx + y_group))
        return 0

    lax.fori_loop(0, 2, beyond, 0)
    q_arrived(beside)
    diagonal(beside)
    full(3, lambda i: (beside, pick(i, group, y_group, 4 + y_group)))
    take("z", 0)
    full(2, lambda i: (pick(i, role, beside), z_group))
    take("far", 0)
    full(2, lambda i: (pick(i, role, beside), far_group))
    q_arrived(flip(1))
    q_arrived(flip(3))

    def others(n, _):
        r = flip(2 * n + 1)
        diagonal(r)
        full(5, lambda i: (r, pick(i, group, y_group, 4 + y_group, z_group, far_group)))

        @pl.when(n == 0)
        def _():
            take("z", 1)

        return 0

    lax.fori_loop(0, 2, others, 0)

    def ending(n, _):
        r = pick(n, zl, 1 - zl, 2 + zl, 3 - zl)

        @pl.when(n == 2)
        def _():
            take("far", 1)

        @pl.when(n >= 2)
        def _():
            full(2, lambda i: (r, 4 + pick(i, z_group, far_group)))

        finish(r)
        return 0

    lax.fori_loop(0, 4, ending, 0)

    for n in range(8):
        wo_load(n).wait()

    def project(d, _):
        r = flip(d)
        for cc in range(2):
            j = cc * 4 + r

            @pl.when(at(r, cc) != dev)
            def _():
                send(os.at[0, 0], orr.at[j], o_s.at[0, 0], o_r.at[j], partner).wait_recv()

        for n in range(8):
            here = slice(n * PIECE, (n + 1) * PIECE)
            t = acc[:, here]
            for cc in range(2):
                j = cc * 4 + r
                t = t + _dot(orr[j], w[(n + 6) % 8, pl.ds(pl.multiple_of(j * PIECE, PIECE), PIECE), :])
            acc[:, here] = t
        return 0

    acc[...] = xs[pl.ds(mine, OWN), :].astype(F32)
    lax.fori_loop(0, 4, project, 0)
    out[...] = acc[...].astype(BF16)
    store = pltpu.make_async_copy(out, y_hbm, out_sem)
    store.start()

    x_send.wait_send()
    for d in (1, 2, 3):
        send(qs.at[d], qr.at[role], q_s.at[d - 1], q_r.at[role], partner).wait_send()

    def left(r, _):
        s, xx = slot(r), lax.div(r, 2)

        @pl.when(along_z(xx))
        def _():
            z_send(s).wait_send()

        @pl.when(along_y(xx))
        def _():
            y_send(s).wait_send()

        came = slot(r, z_group)

        @pl.when(((xx == 0) | (zh == 1) | (py == 0)) & along_y(xx))
        def _():
            send(kv.at[came], kv.at[came], f_s.at[came], kv_r.at[came], y_dev).wait_send()

        for h in range(2):

            @pl.when(at(r, h) != dev)
            def _():
                send(os.at[r, h], orr.at[0], o_s.at[r, h], o_r.at[0], partner).wait_send()

        return 0

    lax.fori_loop(0, 4, left, 0)
    store.wait()


def solution(mesh):
    def step(x, gain, wq, wk, wv, wo):
        half = HEAD // 2
        freq = (THETA ** (-np.arange(half, dtype=np.float32) / half)).astype(np.float32)
        freq = jnp.asarray(np.tile(freq, 2)[None])
        vmem, hbm = pl.BlockSpec(memory_space=pltpu.VMEM), pl.BlockSpec(memory_space=pl.ANY)
        dma = pltpu.SemaphoreType.DMA
        return pl.pallas_call(
            _kernel,
            out_shape=jax.ShapeDtypeStruct((OWN, D), BF16),
            in_specs=[hbm, vmem, vmem, hbm, hbm, hbm, hbm],
            out_specs=hbm,
            scratch_shapes=[
                pltpu.VMEM((8, D, PIECE), BF16),
                pltpu.VMEM((CHIP, D), BF16),
                pltpu.VMEM((CHIP, D), BF16),
                pltpu.VMEM((CHIP, HEAD), F32),
                pltpu.VMEM((CHIP, HEAD), F32),
                pltpu.VMEM((4, 2, CHIP, HEAD), BF16),
                pltpu.VMEM((16, 2, CHIP, HEAD), BF16),
                pltpu.VMEM((4, COLS, HEAD), BF16),
                pltpu.VMEM((4, COLS, HEAD), BF16),
                pltpu.VMEM((4, 8, COLS), F32),
                pltpu.VMEM((4, SUM, COLS), F32),
                pltpu.VMEM((BLOCK, STRIP), jnp.int32),
                pltpu.VMEM((4, 2, OWN, PIECE), BF16),
                pltpu.VMEM((8, OWN, PIECE), BF16),
                pltpu.VMEM((OWN, D), F32),
                pltpu.VMEM((OWN, D), BF16),
                dma, dma((6,)), dma((8,)), dma, dma, dma((3, 2)), dma((4, 2)), dma((16,)), dma((16,)), dma((16,)), dma((16,)), dma((3,)), dma((4,)),
                dma((4, 2)), dma((8,)), dma,
            ],
            compiler_params=pltpu.CompilerParams(collective_id=0, has_side_effects=True, vmem_limit_bytes=63 * 2**20),
        )(x, gain, freq, wq, wk, wv, wo)

    tokens, whole = P(("dp", "sp"), None), P(None, None)
    return jax.shard_map(
        step,
        mesh=mesh,
        in_specs=(tokens, P(None), whole, whole, whole, whole),
        out_specs=tokens,
        check_vma=False,
    )
```

```python
import jax
import jax.numpy as jnp
import numpy as np
from jax import lax
from jax.experimental import pallas as pl
from jax.experimental.pallas import tpu as pltpu
from jax.sharding import PartitionSpec as P

HEAD = 128
THETA = 10000
NEG = -1e30
HIDDEN = 2 * NEG
LOG2E = 1.4426950408889634
E = HEAD**-0.5 * LOG2E
F32, BF16 = jnp.float32, jnp.bfloat16
MESH = pl.DeviceIdType.MESH

OWN = 128
CHIP = 256
D = 4096
G = 4
COLS = G * CHIP
BLOCK = 2 * CHIP
PIECE = 512
STRIP = 512
SUM = HEAD + 8


def _dot(a, b, ca=1, cb=0):
    return lax.dot_general(a, b, (((ca,), (cb,)), ((), ())), preferred_element_type=F32)


def _kernel(x_hbm, gain, freq, wq, wk, wv, wo, y_hbm, w, xs, a, cos, sin, kvs, kv, qs, qr, top, mix, gap, os, orr, acc, out,
            xl_sem, w_sem, wo_sem, xs_sem, xr_sem, kvg_s, kvg_r, kv_r, y_s, z_s, f_s, q_s, q_r, o_s, o_r, out_sem):
    dev = lax.axis_index("sp")
    c = lax.rem(dev, 2)
    chip = lax.div(dev, 2)
    px, py, zh, zl = lax.div(chip, 8), lax.rem(lax.div(chip, 4), 2), lax.rem(lax.div(chip, 2), 2), lax.rem(chip, 2)
    role = px * 2 + zl
    group = py * 2 + zh

    def slot(r, g=group):
        return lax.div(r, 2) * 8 + g * 2 + lax.rem(r, 2)

    def at(r, cc):
        return slot(r) * 2 + cc

    def flip(d):
        dx, dz = (d // 2, d % 2) if isinstance(d, int) else (lax.div(d, 2), lax.rem(d, 2))
        return (px + dx - 2 * px * dx) * 2 + (zl + dz - 2 * zl * dz)

    def send(src, dst, ss, rs, to):
        return pltpu.make_async_remote_copy(src_ref=src, dst_ref=dst, send_sem=ss, recv_sem=rs, device_id={"sp": to}, device_id_type=MESH)

    partner = at(role, 1 - c)
    y_dev = dev + (1 - 2 * py) * 8
    z_dev = dev + (1 - 2 * zh) * 4
    mine = pl.multiple_of(c * OWN, OWN)
    theirs = pl.multiple_of((1 - c) * OWN, OWN)
    cut = pl.multiple_of(c * PIECE, PIECE)

    x_load = pltpu.make_async_copy(x_hbm, xs.at[pl.ds(mine, OWN), :], xl_sem)
    x_load.start()
    wk_load = pltpu.make_async_copy(wk.at[:, pl.ds(cut, PIECE)], w.at[0], w_sem.at[0])
    wv_load = pltpu.make_async_copy(wv.at[:, pl.ds(cut, PIECE)], w.at[1], w_sem.at[1])
    wk_load.start()
    order = (2, 1, 3, 0)

    def q_load(i):
        col = pl.multiple_of((c * 4 + flip(order[i])) * PIECE, PIECE)
        return pltpu.make_async_copy(wq.at[:, pl.ds(col, PIECE)], w.at[2 + i], w_sem.at[2 + i])

    def wo_load(n):
        return pltpu.make_async_copy(wo.at[:, n * PIECE : (n + 1) * PIECE], w.at[(n + 6) % 8], wo_sem.at[n])

    barrier = pltpu.get_barrier_semaphore()

    def greet(to):
        pl.semaphore_signal(barrier, inc=1, device_id={"sp": to}, device_id_type=MESH)

    greet(partner)
    for d in (1, 2, 3):
        greet(at(flip(d), c))
        greet(at(flip(d), 1 - c))
    greet(y_dev)
    greet(z_dev)

    place = (chip * CHIP + lax.broadcasted_iota(jnp.int32, (CHIP, HEAD), 0)).astype(F32)
    angle = place * freq[...]
    cos[...] = jnp.cos(angle)
    turn = jnp.sin(angle)
    sin[...] = jnp.where(lax.broadcasted_iota(jnp.int32, (CHIP, HEAD), 1) < HEAD // 2, -turn, turn)

    x_load.wait()
    wv_load.start()
    pl.semaphore_wait(barrier, 9)

    x_send = send(xs.at[pl.ds(mine, OWN), :], xs.at[pl.ds(mine, OWN), :], xs_sem, xr_sem, partner)
    x_send.start()

    def norm(first):
        def rows(i, _):
            here = pl.ds(pl.multiple_of(first + i * 16, 16), 16)
            wide = xs[here, :].astype(F32)
            scale = lax.rsqrt(jnp.mean(wide * wide, -1, keepdims=True) + 1e-6)
            a[here, :] = (wide * scale * gain[...].astype(F32).reshape(1, D)).astype(BF16)
            return 0

        lax.fori_loop(0, OWN // 16, rows, 0, unroll=2)

    def turned(h, here):
        h = h.astype(BF16).astype(F32)
        return (h * cos[here, :] + pltpu.roll(h, HEAD // 2, 1) * sin[here, :]).astype(BF16)

    def half(d, n):
        return send(kvs.at[flip(d), n], kv.at[chip, n], kvg_s.at[d - 1, n], kvg_r.at[role, n], at(flip(d), c))

    def keys_values(first, n, wait):
        here = pl.ds(first, OWN)
        t = _dot(a[here, :], w[0])
        for j in range(4):
            kvs[j, n, :OWN, :] = turned(t[:, j * HEAD : (j + 1) * HEAD], here)
        if wait:
            wv_load.wait()
        t = _dot(a[here, :], w[1])
        for j in range(4):
            kvs[j, n, OWN:, :] = t[:, j * HEAD : (j + 1) * HEAD].T.astype(BF16)
        for d in (1, 2, 3):
            half(d, n).start()

    norm(mine)
    wk_load.wait()
    for i in range(4):
        q_load(i).start()
    wo_load(0).start()
    wo_load(1).start()
    keys_values(mine, c, True)
    send(xs.at[pl.ds(theirs, OWN), :], xs.at[pl.ds(theirs, OWN), :], xs_sem, xr_sem, partner).wait_recv()
    norm(theirs)
    keys_values(theirs, 1 - c, False)
    wo_load(2).start()
    wo_load(3).start()

    kv[chip] = kvs[role]

    def along_y(xx):
        return (xx == 0) | (py == 0)

    def along_z(xx):
        return (xx == 0) | (zh == 0) | (py == 0)

    def y_send(s):
        return send(kv.at[s], kv.at[s], y_s.at[s], kv_r.at[s], y_dev)

    def z_send(s):
        return send(kv.at[s], kv.at[s], z_s.at[s], kv_r.at[s], z_dev)

    def arrived(s):
        send(kv.at[s], kv.at[s], y_s.at[s], kv_r.at[s], partner).wait_recv()

    def half_arrived(r, n):
        send(kvs.at[0, 0], kv.at[slot(r), n], kvg_s.at[0, 0], kvg_r.at[r, n], partner).wait_recv()

    def share_z(r, xx):
        @pl.when((lax.div(r, 2) == xx) & along_z(xx))
        def _():
            z_send(slot(r)).start()

    def share(r):
        share_z(r, 0)

        @pl.when(along_y(lax.div(r, 2)))
        def _():
            y_send(slot(r)).start()

    share(role)

    mix[...] = jnp.zeros_like(mix)
    top[...] = jnp.full_like(top, NEG)
    gap[...] = lax.rem(lax.broadcasted_iota(jnp.int32, (BLOCK, STRIP), 1), CHIP) - lax.broadcasted_iota(jnp.int32, (BLOCK, STRIP), 0)

    for i in range(4):
        d = order[i]
        q_load(i).wait()
        t = _dot(a[...], w[2 + i])
        dst = qr.at[role] if d == 0 else qs.at[d]
        for g in range(G):
            dst[g * CHIP : (g + 1) * CHIP, :] = turned(t[:, g * HEAD : (g + 1) * HEAD], slice(None))
        wo_load(4 + i).start()
        for n in ((), (1, 2), (3,), ())[i]:
            for h in range(2):
                half_arrived(flip(n), h)
            share(flip(n))
        if d:
            send(qs.at[d], qr.at[role], q_s.at[d - 1], q_r.at[role], at(flip(d), c)).start()

    ones = jnp.ones((8, BLOCK), BF16)

    def items(tasks, masked=False):
        strips = []
        for r, m in tasks:
            halves = [kv[2 * m + i, n] for i in range(2) for n in range(2)]
            keys = jnp.concatenate([h[:OWN] for h in halves], axis=0)
            values = jnp.concatenate([h[OWN:] for h in halves], axis=1)
            values = jnp.concatenate([values, ones], axis=0)
            strips += [(r, keys, values, slice(i, i + STRIP)) for i in range(0, COLS, STRIP)]
        scores = [_dot(keys, qr[r, cols, :], 1, 1) for r, keys, _, cols in strips]
        weights, keeps = [], []
        for (r, _, _, cols), v in zip(strips, scores):
            if masked:
                v = jnp.where(gap[...] >= -CHIP * lax.rem(r, 2), v, HIDDEN)
            old = top[r, 0:1, cols]
            new = jnp.maximum(old, v.max(axis=0, keepdims=True))
            top[r, 0:1, cols] = new
            weights.append(jnp.exp2((v - new) * E).astype(BF16))
            keeps.append(jnp.exp2((old - new) * E))
        for (r, _, values, cols), v, keep in zip(strips, weights, keeps):
            mix[r, :, cols] = mix[r, :, cols] * keep + _dot(values, v)

    y_group, z_group, far_group = (1 - py) * 2 + zh, py * 2 + 1 - zh, (1 - py) * 2 + 1 - zh

    def take(g, xx):
        sent = {"y": (xx == 0) | (py == 1), "z": (xx == 0) | (zh == 1) | (py == 0), "far": (xx == 0) | (py == 1)}[g]
        number = {"y": y_group, "z": z_group, "far": far_group}[g]

        @pl.when(sent)
        def _():
            for n in range(2):
                s = slot(xx * 2 + n, number)
                arrived(s)
                if g == "z":

                    @pl.when(along_y(xx))
                    def _():
                        send(kv.at[s], kv.at[s], f_s.at[s], kv_r.at[s], y_dev).start()

    def q_arrived(r):
        send(qs.at[1], qr.at[r], q_s.at[0], q_r.at[r], partner).wait_recv()

    def counts(r, m):
        return m < lax.div(r, 2) * 4 + group

    def single(r, m):
        @pl.when(counts(r, m))
        def _():
            items([(r, m)])

    def full(n, task):
        lax.fori_loop(0, n, lambda i, _: (single(*task(i)), 0)[1], 0)

    def both(n, task):
        def one(i, _):
            first, second = task(i)

            @pl.when(counts(*second))
            def _():
                items([first, second])

            @pl.when(jnp.logical_not(counts(*second)))
            def _():
                single(*first)

            return 0

        lax.fori_loop(0, n, one, 0)

    def pick(i, *choices):
        got = choices[-1]
        for n in range(len(choices) - 2, -1, -1):
            got = jnp.where(i == n, choices[n], got)
        return got

    def diagonal(r):
        items([(r, lax.div(r, 2) * 4 + group)], True)

    def finish(r):
        o = mix[r, :HEAD, :] * (1 / mix[r, HEAD : HEAD + 1, :])
        for g in range(G):
            for h in range(2):
                first = g * CHIP + h * OWN
                os[r, h, :, g * HEAD : (g + 1) * HEAD] = o[:, first : first + OWN].T.astype(BF16)
        for h in range(2):
            to = at(r, h)

            @pl.when(to != dev)
            def _():
                send(os.at[r, h], orr.at[c * 4 + role], o_s.at[r, h], o_r.at[c * 4 + role], to).start()

            @pl.when(to == dev)
            def _():
                orr[c * 4 + role] = os[r, h]

    beside = flip(2)
    diagonal(role)
    full(1, lambda i: (role, group))

    def beyond(i, _):
        xx = jnp.where(i == 0, px, 1 - px)
        take("y", xx)
        full(1, lambda i: (role, 4 * xx + y_group))
        return 0

    lax.fori_loop(0, 2, beyond, 0)
    for d in range(4):
        share_z(flip(d), 1)
    q_arrived(beside)
    diagonal(beside)
    full(3, lambda i: (beside, pick(i, group, y_group, 4 + y_group)))
    take("z", 0)
    both(1, lambda i: ((2 + zl, z_group), (zl, z_group)))
    take("far", 0)
    both(1, lambda i: ((2 + zl, far_group), (zl, far_group)))
    finish(zl)

    r0, r1 = 1 - zl, 3 - zl
    q_arrived(r0)
    q_arrived(r1)
    items([(r0, group), (r1, 4 + group)], True)
    both(3, lambda i: ((r1, pick(i, y_group, z_group, far_group)), (r0, pick(i, y_group, z_group, far_group))))
    finish(r0)
    both(1, lambda i: ((r1, group), (r1, 4 + y_group)))

    def late(i, _):
        @pl.when(i == 0)
        def _():
            take("z", 1)

        @pl.when(i == 1)
        def _():
            take("far", 1)

        m = 4 + pick(i, z_group, far_group)

        @pl.when(counts(r1, m))
        def _():
            items([(r1, m), (2 + zl, m)])

        return 0

    lax.fori_loop(0, 2, late, 0)
    lax.fori_loop(0, 2, lambda i, _: (finish(pick(i, r1, 2 + zl)), 0)[1], 0)

    for n in range(8):
        wo_load(n).wait()

    def store(n):
        here = slice(n * PIECE, (n + 1) * PIECE)
        return pltpu.make_async_copy(out.at[:, here], y_hbm.at[:, here], out_sem.at[n])

    def project(r, last):
        for cc in range(2):
            j = cc * 4 + r

            @pl.when(at(r, cc) != dev)
            def _():
                send(os.at[0, 0], orr.at[j], o_s.at[0, 0], o_r.at[j], partner).wait_recv()

        for n in range(8):
            here = slice(n * PIECE, (n + 1) * PIECE)
            t = acc[:, here]
            for cc in range(2):
                j = cc * 4 + r
                t = t + _dot(orr[j], w[(n + 6) % 8, pl.ds(pl.multiple_of(j * PIECE, PIECE), PIECE), :])
            if last:
                out[:, here] = t.astype(BF16)
                store(n).start()
            else:
                acc[:, here] = t

    acc[...] = xs[pl.ds(mine, OWN), :].astype(F32)
    lax.fori_loop(0, 3, lambda n, _: (project(flip(pick(n, 0, 2, 1)), False), 0)[1], 0)
    project(flip(3), True)

    x_send.wait_send()
    for d in (1, 2, 3):
        for n in range(2):
            half(d, n).wait_send()
        send(qs.at[d], qr.at[role], q_s.at[d - 1], q_r.at[role], partner).wait_send()

    def left(r, _):
        s, xx = slot(r), lax.div(r, 2)

        @pl.when(along_z(xx))
        def _():
            z_send(s).wait_send()

        @pl.when(along_y(xx))
        def _():
            y_send(s).wait_send()

        came = slot(r, z_group)

        @pl.when(((xx == 0) | (zh == 1) | (py == 0)) & along_y(xx))
        def _():
            send(kv.at[came], kv.at[came], f_s.at[came], kv_r.at[came], y_dev).wait_send()

        for h in range(2):

            @pl.when(at(r, h) != dev)
            def _():
                send(os.at[r, h], orr.at[0], o_s.at[r, h], o_r.at[0], partner).wait_send()

        return 0

    lax.fori_loop(0, 4, left, 0)
    for n in range(8):
        store(n).wait()


def solution(mesh):
    def step(x, gain, wq, wk, wv, wo):
        half = HEAD // 2
        freq = (THETA ** (-np.arange(half, dtype=np.float32) / half)).astype(np.float32)
        freq = jnp.asarray(np.tile(freq, 2)[None])
        vmem, hbm = pl.BlockSpec(memory_space=pltpu.VMEM), pl.BlockSpec(memory_space=pl.ANY)
        dma = pltpu.SemaphoreType.DMA
        return pl.pallas_call(
            _kernel,
            out_shape=jax.ShapeDtypeStruct((OWN, D), BF16),
            in_specs=[hbm, vmem, vmem, hbm, hbm, hbm, hbm],
            out_specs=hbm,
            scratch_shapes=[
                pltpu.VMEM((8, D, PIECE), BF16),
                pltpu.VMEM((CHIP, D), BF16),
                pltpu.VMEM((CHIP, D), BF16),
                pltpu.VMEM((CHIP, HEAD), F32),
                pltpu.VMEM((CHIP, HEAD), F32),
                pltpu.VMEM((4, 2, CHIP, HEAD), BF16),
                pltpu.VMEM((16, 2, CHIP, HEAD), BF16),
                pltpu.VMEM((4, COLS, HEAD), BF16),
                pltpu.VMEM((4, COLS, HEAD), BF16),
                pltpu.VMEM((4, 8, COLS), F32),
                pltpu.VMEM((4, SUM, COLS), F32),
                pltpu.VMEM((BLOCK, STRIP), jnp.int32),
                pltpu.VMEM((4, 2, OWN, PIECE), BF16),
                pltpu.VMEM((8, OWN, PIECE), BF16),
                pltpu.VMEM((OWN, D), F32),
                pltpu.VMEM((OWN, D), BF16),
                dma, dma((6,)), dma((8,)), dma, dma, dma((3, 2)), dma((4, 2)), dma((16,)), dma((16,)), dma((16,)), dma((16,)), dma((3,)), dma((4,)),
                dma((4, 2)), dma((8,)), dma((8,)),
            ],
            compiler_params=pltpu.CompilerParams(collective_id=0, has_side_effects=True, vmem_limit_bytes=63 * 2**20),
        )(x, gain, freq, wq, wk, wv, wo)

    tokens, whole = P(("dp", "sp"), None), P(None, None)
    return jax.shard_map(
        step,
        mesh=mesh,
        in_specs=(tokens, P(None), whole, whole, whole, whole),
        out_specs=tokens,
        check_vma=False,
    )
```

```python
import jax
import jax.numpy as jnp
import numpy as np
from jax import lax
from jax.experimental import pallas as pl
from jax.experimental.pallas import tpu as pltpu
from jax.sharding import PartitionSpec as P

HEAD = 128
THETA = 10000
NEG = -1e30
HIDDEN = 2 * NEG
LOG2E = 1.4426950408889634
E = HEAD**-0.5 * LOG2E
F32, BF16 = jnp.float32, jnp.bfloat16
MESH = pl.DeviceIdType.MESH

OWN = 128
CHIP = 256
D = 4096
G = 4
COLS = G * CHIP
BLOCK = 2 * CHIP
PIECE = 512
STRIP = 512
SUM = HEAD + 8


def _dot(a, b, ca=1, cb=0):
    return lax.dot_general(a, b, (((ca,), (cb,)), ((), ())), preferred_element_type=F32)


def _kernel(x_hbm, gain, freq, wq, wk, wv, wo, out, w, xs, a, cos, sin, kvs, kv, qs, qr, top, mix, gap, os, orr, acc,
            xl_sem, w_sem, wo_sem, xs_sem, xr_sem, kvg_s, kvg_r, kv_r, y_s, z_s, f_s, q_s, q_r, o_s, o_r):
    dev = lax.axis_index("sp")
    c = lax.rem(dev, 2)
    chip = lax.div(dev, 2)
    px, py, zh, zl = lax.div(chip, 8), lax.rem(lax.div(chip, 4), 2), lax.rem(lax.div(chip, 2), 2), lax.rem(chip, 2)
    role = px * 2 + zl
    group = py * 2 + zh

    def slot(r, g=group):
        return lax.div(r, 2) * 8 + g * 2 + lax.rem(r, 2)

    def at(r, cc):
        return slot(r) * 2 + cc

    def flip(d):
        dx, dz = (d // 2, d % 2) if isinstance(d, int) else (lax.div(d, 2), lax.rem(d, 2))
        return (px + dx - 2 * px * dx) * 2 + (zl + dz - 2 * zl * dz)

    def send(src, dst, ss, rs, to):
        return pltpu.make_async_remote_copy(src_ref=src, dst_ref=dst, send_sem=ss, recv_sem=rs, device_id={"sp": to}, device_id_type=MESH)

    partner = at(role, 1 - c)
    y_dev = dev + (1 - 2 * py) * 8
    z_dev = dev + (1 - 2 * zh) * 4
    mine = pl.multiple_of(c * OWN, OWN)
    theirs = pl.multiple_of((1 - c) * OWN, OWN)
    cut = pl.multiple_of(c * PIECE, PIECE)

    x_load = pltpu.make_async_copy(x_hbm, xs.at[pl.ds(mine, OWN), :], xl_sem)
    x_load.start()
    wk_load = pltpu.make_async_copy(wk.at[:, pl.ds(cut, PIECE)], w.at[0], w_sem.at[0])
    wv_load = pltpu.make_async_copy(wv.at[:, pl.ds(cut, PIECE)], w.at[1], w_sem.at[1])
    wk_load.start()
    order = (2, 1, 3, 0)

    def q_load(i):
        col = pl.multiple_of((c * 4 + flip(order[i])) * PIECE, PIECE)
        return pltpu.make_async_copy(wq.at[:, pl.ds(col, PIECE)], w.at[2 + i], w_sem.at[2 + i])

    def wo_load(n):
        return pltpu.make_async_copy(wo.at[:, n * PIECE : (n + 1) * PIECE], w.at[(n + 6) % 8], wo_sem.at[n])

    barrier = pltpu.get_barrier_semaphore()

    def greet(to):
        pl.semaphore_signal(barrier, inc=1, device_id={"sp": to}, device_id_type=MESH)

    greet(partner)
    for d in (1, 2, 3):
        greet(at(flip(d), c))
        greet(at(flip(d), 1 - c))
    greet(y_dev)
    greet(z_dev)

    place = (chip * CHIP + lax.broadcasted_iota(jnp.int32, (CHIP, HEAD), 0)).astype(F32)
    angle = place * freq[...]
    cos[...] = jnp.cos(angle)
    turn = jnp.sin(angle)
    sin[...] = jnp.where(lax.broadcasted_iota(jnp.int32, (CHIP, HEAD), 1) < HEAD // 2, -turn, turn)

    wv_load.start()
    x_load.wait()
    pl.semaphore_wait(barrier, 9)

    x_send = send(xs.at[pl.ds(mine, OWN), :], xs.at[pl.ds(mine, OWN), :], xs_sem, xr_sem, partner)
    x_send.start()

    def norm(first):
        def rows(i, _):
            here = pl.ds(pl.multiple_of(first + i * 16, 16), 16)
            wide = xs[here, :].astype(F32)
            scale = lax.rsqrt(jnp.mean(wide * wide, -1, keepdims=True) + 1e-6)
            a[here, :] = (wide * scale * gain[...].astype(F32).reshape(1, D)).astype(BF16)
            return 0

        lax.fori_loop(0, OWN // 16, rows, 0, unroll=2)

    def turned(h, here):
        h = h.astype(BF16).astype(F32)
        return (h * cos[here, :] + pltpu.roll(h, HEAD // 2, 1) * sin[here, :]).astype(BF16)

    def half(d, n):
        return send(kvs.at[flip(d), n], kv.at[chip, n], kvg_s.at[d - 1, n], kvg_r.at[role, n], at(flip(d), c))

    def keys_values(first, n, wait):
        here = pl.ds(first, OWN)
        t = _dot(a[here, :], w[0])
        for j in range(4):
            kvs[j, n, :OWN, :] = turned(t[:, j * HEAD : (j + 1) * HEAD], here)
        if wait:
            wv_load.wait()
        t = _dot(a[here, :], w[1])
        for j in range(4):
            kvs[j, n, OWN:, :] = t[:, j * HEAD : (j + 1) * HEAD].T.astype(BF16)
        for d in (1, 2, 3):
            half(d, n).start()

    norm(mine)
    wk_load.wait()
    for i in range(4):
        q_load(i).start()
    wo_load(0).start()
    wo_load(1).start()
    keys_values(mine, c, True)
    send(xs.at[pl.ds(theirs, OWN), :], xs.at[pl.ds(theirs, OWN), :], xs_sem, xr_sem, partner).wait_recv()
    norm(theirs)
    keys_values(theirs, 1 - c, False)
    wo_load(2).start()
    wo_load(3).start()

    kv[chip] = kvs[role]

    def along_y(xx):
        return (xx == 0) | (py == 0)

    def along_z(xx):
        return (xx == 0) | (zh == 0) | (py == 0)

    def y_send(s):
        return send(kv.at[s], kv.at[s], y_s.at[s], kv_r.at[s], y_dev)

    def z_send(s):
        return send(kv.at[s], kv.at[s], z_s.at[s], kv_r.at[s], z_dev)

    def arrived(s):
        send(kv.at[s], kv.at[s], y_s.at[s], kv_r.at[s], partner).wait_recv()

    def half_arrived(r, n):
        send(kvs.at[0, 0], kv.at[slot(r), n], kvg_s.at[0, 0], kvg_r.at[r, n], partner).wait_recv()

    def share_z(r, xx):
        @pl.when((lax.div(r, 2) == xx) & along_z(xx))
        def _():
            z_send(slot(r)).start()

    def share(r):
        share_z(r, 0)

        @pl.when(along_y(lax.div(r, 2)))
        def _():
            y_send(slot(r)).start()

    share(role)

    mix[...] = jnp.zeros_like(mix)
    top[...] = jnp.full_like(top, NEG)
    gap[...] = lax.rem(lax.broadcasted_iota(jnp.int32, (BLOCK, STRIP), 1), CHIP) - lax.broadcasted_iota(jnp.int32, (BLOCK, STRIP), 0)

    for i in range(4):
        d = order[i]
        q_load(i).wait()
        t = _dot(a[...], w[2 + i])
        dst = qr.at[role] if d == 0 else qs.at[d]
        for g in range(G):
            dst[g * CHIP : (g + 1) * CHIP, :] = turned(t[:, g * HEAD : (g + 1) * HEAD], slice(None))
        wo_load(4 + i).start()
        for n in ((), (1, 2), (3,), ())[i]:
            for h in range(2):
                half_arrived(flip(n), h)
            share(flip(n))
        if d:
            send(qs.at[d], qr.at[role], q_s.at[d - 1], q_r.at[role], at(flip(d), c)).start()

    ones = jnp.ones((8, BLOCK), BF16)

    def items(tasks, masked=False):
        strips = []
        for r, m in tasks:
            halves = [kv[2 * m + i, n] for i in range(2) for n in range(2)]
            keys = jnp.concatenate([h[:OWN] for h in halves], axis=0)
            values = jnp.concatenate([h[OWN:] for h in halves], axis=1)
            values = jnp.concatenate([values, ones], axis=0)
            strips += [(r, keys, values, slice(i, i + STRIP)) for i in range(0, COLS, STRIP)]
        scores = [_dot(keys, qr[r, cols, :], 1, 1) for r, keys, _, cols in strips]
        weights, keeps = [], []
        for (r, _, _, cols), v in zip(strips, scores):
            if masked:
                v = jnp.where(gap[...] >= -CHIP * lax.rem(r, 2), v, HIDDEN)
            old = top[r, 0:1, cols]
            new = jnp.maximum(old, v.max(axis=0, keepdims=True))
            top[r, 0:1, cols] = new
            weights.append(jnp.exp2((v - new) * E).astype(BF16))
            keeps.append(jnp.exp2((old - new) * E))
        for (r, _, values, cols), v, keep in zip(strips, weights, keeps):
            mix[r, :, cols] = mix[r, :, cols] * keep + _dot(values, v)

    y_group, z_group, far_group = (1 - py) * 2 + zh, py * 2 + 1 - zh, (1 - py) * 2 + 1 - zh

    def take(g, xx):
        sent = {"y": (xx == 0) | (py == 1), "z": (xx == 0) | (zh == 1) | (py == 0), "far": (xx == 0) | (py == 1)}[g]
        number = {"y": y_group, "z": z_group, "far": far_group}[g]

        @pl.when(sent)
        def _():
            for n in range(2):
                s = slot(xx * 2 + n, number)
                arrived(s)
                if g == "z":

                    @pl.when(along_y(xx))
                    def _():
                        send(kv.at[s], kv.at[s], f_s.at[s], kv_r.at[s], y_dev).start()

    def q_arrived(r):
        send(qs.at[1], qr.at[r], q_s.at[0], q_r.at[r], partner).wait_recv()

    def counts(r, m):
        return m < lax.div(r, 2) * 4 + group

    def single(r, m):
        @pl.when(counts(r, m))
        def _():
            items([(r, m)])

    def full(n, task):
        lax.fori_loop(0, n, lambda i, _: (single(*task(i)), 0)[1], 0)

    def both(n, task):
        def one(i, _):
            first, second = task(i)

            @pl.when(counts(*second))
            def _():
                items([first, second])

            @pl.when(jnp.logical_not(counts(*second)))
            def _():
                single(*first)

            return 0

        lax.fori_loop(0, n, one, 0)

    def pick(i, *choices):
        got = choices[-1]
        for n in range(len(choices) - 2, -1, -1):
            got = jnp.where(i == n, choices[n], got)
        return got

    def diagonal(r):
        items([(r, lax.div(r, 2) * 4 + group)], True)

    def finish(r):
        o = mix[r, :HEAD, :] * (1 / mix[r, HEAD : HEAD + 1, :])
        for g in range(G):
            for h in range(2):
                first = g * CHIP + h * OWN
                os[r, h, :, g * HEAD : (g + 1) * HEAD] = o[:, first : first + OWN].T.astype(BF16)
        for h in range(2):
            to = at(r, h)

            @pl.when(to != dev)
            def _():
                send(os.at[r, h], orr.at[c * 4 + role], o_s.at[r, h], o_r.at[c * 4 + role], to).start()

            @pl.when(to == dev)
            def _():
                orr[c * 4 + role] = os[r, h]

    beside = flip(2)
    diagonal(role)
    full(1, lambda i: (role, group))

    def beyond(i, _):
        xx = jnp.where(i == 0, px, 1 - px)
        take("y", xx)
        full(1, lambda i: (role, 4 * xx + y_group))
        return 0

    lax.fori_loop(0, 2, beyond, 0)
    for d in range(4):
        share_z(flip(d), 1)
    q_arrived(beside)
    diagonal(beside)
    full(3, lambda i: (beside, pick(i, group, y_group, 4 + y_group)))
    take("z", 0)
    both(1, lambda i: ((2 + zl, z_group), (zl, z_group)))
    take("far", 0)
    both(1, lambda i: ((2 + zl, far_group), (zl, far_group)))
    finish(zl)

    r0, r1 = 1 - zl, 3 - zl

    @pl.when(py == 0)
    def _():
        take("z", 1)

    q_arrived(r0)
    q_arrived(r1)
    items([(r0, group), (r1, 4 + group)], True)
    both(3, lambda i: ((r1, pick(i, y_group, z_group, far_group)), (r0, pick(i, y_group, z_group, far_group))))
    finish(r0)
    both(1, lambda i: ((r1, group), (r1, 4 + y_group)))

    def late(i, _):
        @pl.when((i == 0) & (py == 1))
        def _():
            take("z", 1)

        @pl.when(i == 1)
        def _():
            take("far", 1)

        m = 4 + pick(i, z_group, far_group)

        @pl.when(counts(r1, m))
        def _():
            items([(r1, m), (2 + zl, m)])

        return 0

    lax.fori_loop(0, 2, late, 0)
    lax.fori_loop(0, 2, lambda i, _: (finish(pick(i, r1, 2 + zl)), 0)[1], 0)

    for n in range(8):
        wo_load(n).wait()

    def project(r, last):
        for cc in range(2):
            j = cc * 4 + r

            @pl.when(at(r, cc) != dev)
            def _():
                send(os.at[0, 0], orr.at[j], o_s.at[0, 0], o_r.at[j], partner).wait_recv()

        for n in range(8):
            here = slice(n * PIECE, (n + 1) * PIECE)
            t = acc[:, here]
            for cc in range(2):
                j = cc * 4 + r
                t = t + _dot(orr[j], w[(n + 6) % 8, pl.ds(pl.multiple_of(j * PIECE, PIECE), PIECE), :])
            if last:
                out[:, here] = t.astype(BF16)
            else:
                acc[:, here] = t

    acc[...] = xs[pl.ds(mine, OWN), :].astype(F32)
    lax.fori_loop(0, 3, lambda n, _: (project(flip(pick(n, 0, 2, 1)), False), 0)[1], 0)
    project(flip(3), True)

    x_send.wait_send()
    for d in (1, 2, 3):
        for n in range(2):
            half(d, n).wait_send()
        send(qs.at[d], qr.at[role], q_s.at[d - 1], q_r.at[role], partner).wait_send()

    def left(r, _):
        s, xx = slot(r), lax.div(r, 2)

        @pl.when(along_z(xx))
        def _():
            z_send(s).wait_send()

        @pl.when(along_y(xx))
        def _():
            y_send(s).wait_send()

        came = slot(r, z_group)

        @pl.when(((xx == 0) | (zh == 1) | (py == 0)) & along_y(xx))
        def _():
            send(kv.at[came], kv.at[came], f_s.at[came], kv_r.at[came], y_dev).wait_send()

        for h in range(2):

            @pl.when(at(r, h) != dev)
            def _():
                send(os.at[r, h], orr.at[0], o_s.at[r, h], o_r.at[0], partner).wait_send()

        return 0

    lax.fori_loop(0, 4, left, 0)


def solution(mesh):
    def step(x, gain, wq, wk, wv, wo):
        half = HEAD // 2
        freq = (THETA ** (-np.arange(half, dtype=np.float32) / half)).astype(np.float32)
        freq = jnp.asarray(np.tile(freq, 2)[None])
        vmem, hbm = pl.BlockSpec(memory_space=pltpu.VMEM), pl.BlockSpec(memory_space=pl.ANY)
        dma = pltpu.SemaphoreType.DMA
        return pl.pallas_call(
            _kernel,
            out_shape=pltpu.VMEM((OWN, D), BF16),
            in_specs=[hbm, vmem, vmem, hbm, hbm, hbm, hbm],
            out_specs=vmem,
            scratch_shapes=[
                pltpu.VMEM((8, D, PIECE), BF16),
                pltpu.VMEM((CHIP, D), BF16),
                pltpu.VMEM((CHIP, D), BF16),
                pltpu.VMEM((CHIP, HEAD), F32),
                pltpu.VMEM((CHIP, HEAD), F32),
                pltpu.VMEM((4, 2, CHIP, HEAD), BF16),
                pltpu.VMEM((16, 2, CHIP, HEAD), BF16),
                pltpu.VMEM((4, COLS, HEAD), BF16),
                pltpu.VMEM((4, COLS, HEAD), BF16),
                pltpu.VMEM((4, 8, COLS), F32),
                pltpu.VMEM((4, SUM, COLS), F32),
                pltpu.VMEM((BLOCK, STRIP), jnp.int32),
                pltpu.VMEM((4, 2, OWN, PIECE), BF16),
                pltpu.VMEM((8, OWN, PIECE), BF16),
                pltpu.VMEM((OWN, D), F32),
                dma, dma((6,)), dma((8,)), dma, dma, dma((3, 2)), dma((4, 2)), dma((16,)), dma((16,)), dma((16,)), dma((16,)), dma((3,)), dma((4,)),
                dma((4, 2)), dma((8,)),
            ],
            compiler_params=pltpu.CompilerParams(collective_id=0, has_side_effects=True, vmem_limit_bytes=60 * 2**20),
        )(x, gain, freq, wq, wk, wv, wo)

    tokens, whole = P(("dp", "sp"), None), P(None, None)
    return jax.shard_map(
        step,
        mesh=mesh,
        in_specs=(tokens, P(None), whole, whole, whole, whole),
        out_specs=tokens,
        check_vma=False,
    )
```

```python
import jax
import jax.numpy as jnp
import numpy as np
from jax import lax
from jax.experimental import pallas as pl
from jax.experimental.pallas import tpu as pltpu
from jax.sharding import PartitionSpec as P

HEAD = 128
THETA = 10000
NEG = -1e30
HIDDEN = 2 * NEG
LOG2E = 1.4426950408889634
E = HEAD**-0.5 * LOG2E
F32, BF16 = jnp.float32, jnp.bfloat16
MESH = pl.DeviceIdType.MESH

OWN = 128
CHIP = 256
D = 4096
G = 4
COLS = G * CHIP
BLOCK = 2 * CHIP
PIECE = 512
STRIP = 512
SUM = HEAD + 8


def _dot(a, b, ca=1, cb=0):
    return lax.dot_general(a, b, (((ca,), (cb,)), ((), ())), preferred_element_type=F32)


def _kernel(x_hbm, gain, freq, wq, wk, wv, wo, out, w, xs, a, cos, sin, kvs, kv, qs, qr, top, mix, gap, os, orr, acc,
            xl_sem, w_sem, wo_sem, xs_sem, xr_sem, kvg_s, kvg_r, kv_r, y_s, z_s, f_s, q_s, q_r, o_s, o_r):
    dev = lax.axis_index("sp")
    c = lax.rem(dev, 2)
    chip = lax.div(dev, 2)
    px, py, zh, zl = lax.div(chip, 8), lax.rem(lax.div(chip, 4), 2), lax.rem(lax.div(chip, 2), 2), lax.rem(chip, 2)
    role = px * 2 + zl
    group = py * 2 + zh

    def slot(r, g=group):
        return lax.div(r, 2) * 8 + g * 2 + lax.rem(r, 2)

    def at(r, cc):
        return slot(r) * 2 + cc

    def flip(d):
        dx, dz = (d // 2, d % 2) if isinstance(d, int) else (lax.div(d, 2), lax.rem(d, 2))
        return (px + dx - 2 * px * dx) * 2 + (zl + dz - 2 * zl * dz)

    def send(src, dst, ss, rs, to):
        return pltpu.make_async_remote_copy(src_ref=src, dst_ref=dst, send_sem=ss, recv_sem=rs, device_id={"sp": to}, device_id_type=MESH)

    partner = at(role, 1 - c)
    y_dev = dev + (1 - 2 * py) * 8
    z_dev = dev + (1 - 2 * zh) * 4
    mine = pl.multiple_of(c * OWN, OWN)
    theirs = pl.multiple_of((1 - c) * OWN, OWN)
    cut = pl.multiple_of(c * PIECE, PIECE)

    x_load = pltpu.make_async_copy(x_hbm, xs.at[pl.ds(mine, OWN), :], xl_sem)
    x_load.start()
    wk_load = pltpu.make_async_copy(wk.at[:, pl.ds(cut, PIECE)], w.at[0], w_sem.at[0])
    wv_load = pltpu.make_async_copy(wv.at[:, pl.ds(cut, PIECE)], w.at[1], w_sem.at[1])
    wk_load.start()
    order = (2, 1, 3, 0)

    def q_load(i):
        col = pl.multiple_of((c * 4 + flip(order[i])) * PIECE, PIECE)
        return pltpu.make_async_copy(wq.at[:, pl.ds(col, PIECE)], w.at[2 + i], w_sem.at[2 + i])

    def wo_load(n):
        return pltpu.make_async_copy(wo.at[:, n * PIECE : (n + 1) * PIECE], w.at[(n + 6) % 8], wo_sem.at[n])

    barrier = pltpu.get_barrier_semaphore()

    def greet(to):
        pl.semaphore_signal(barrier, inc=1, device_id={"sp": to}, device_id_type=MESH)

    greet(partner)
    for d in (1, 2, 3):
        greet(at(flip(d), c))
        greet(at(flip(d), 1 - c))
    greet(y_dev)
    greet(z_dev)

    place = (chip * CHIP + lax.broadcasted_iota(jnp.int32, (CHIP, HEAD), 0)).astype(F32)
    angle = place * freq[...]
    cos[...] = jnp.cos(angle)
    turn = jnp.sin(angle)
    sin[...] = jnp.where(lax.broadcasted_iota(jnp.int32, (CHIP, HEAD), 1) < HEAD // 2, -turn, turn)

    wv_load.start()
    x_load.wait()
    pl.semaphore_wait(barrier, 9)

    x_send = send(xs.at[pl.ds(mine, OWN), :], xs.at[pl.ds(mine, OWN), :], xs_sem, xr_sem, partner)
    x_send.start()

    def norm(first):
        def rows(i, _):
            here = pl.ds(pl.multiple_of(first + i * 16, 16), 16)
            wide = xs[here, :].astype(F32)
            scale = lax.rsqrt(jnp.mean(wide * wide, -1, keepdims=True) + 1e-6)
            a[here, :] = (wide * scale * gain[...].astype(F32).reshape(1, D)).astype(BF16)
            return 0

        lax.fori_loop(0, OWN // 16, rows, 0, unroll=2)

    def turned(h, here):
        h = h.astype(BF16).astype(F32)
        return (h * cos[here, :] + pltpu.roll(h, HEAD // 2, 1) * sin[here, :]).astype(BF16)

    def half(d, n):
        return send(kvs.at[flip(d), n], kv.at[chip, n], kvg_s.at[d - 1, n], kvg_r.at[role, n], at(flip(d), c))

    def keys_values(first, n, wait):
        here = pl.ds(first, OWN)
        t = _dot(a[here, :], w[0])
        for j in range(4):
            kvs[j, n, :OWN, :] = turned(t[:, j * HEAD : (j + 1) * HEAD], here)
        if wait:
            wv_load.wait()
        t = _dot(a[here, :], w[1])
        for j in range(4):
            kvs[j, n, OWN:, :] = t[:, j * HEAD : (j + 1) * HEAD].T.astype(BF16)
        for d in (1, 2, 3):
            half(d, n).start()

    norm(mine)
    wk_load.wait()
    for i in range(4):
        q_load(i).start()
    wo_load(0).start()
    wo_load(1).start()
    keys_values(mine, c, True)
    send(xs.at[pl.ds(theirs, OWN), :], xs.at[pl.ds(theirs, OWN), :], xs_sem, xr_sem, partner).wait_recv()
    norm(theirs)
    keys_values(theirs, 1 - c, False)
    wo_load(2).start()
    wo_load(3).start()

    kv[chip] = kvs[role]

    def along_y(xx):
        return (xx == 0) | (py == 0)

    def along_z(xx):
        return (xx == 0) | (zh == 0) | (py == 0)

    def y_send(s):
        return send(kv.at[s], kv.at[s], y_s.at[s], kv_r.at[s], y_dev)

    def z_send(s):
        return send(kv.at[s], kv.at[s], z_s.at[s], kv_r.at[s], z_dev)

    def arrived(s):
        send(kv.at[s], kv.at[s], y_s.at[s], kv_r.at[s], partner).wait_recv()

    def half_arrived(r, n):
        send(kvs.at[0, 0], kv.at[slot(r), n], kvg_s.at[0, 0], kvg_r.at[r, n], partner).wait_recv()

    def share_z(r, xx):
        @pl.when((lax.div(r, 2) == xx) & along_z(xx))
        def _():
            z_send(slot(r)).start()

    def share(r):
        share_z(r, 0)

        @pl.when(along_y(lax.div(r, 2)))
        def _():
            y_send(slot(r)).start()

    share(role)

    mix[...] = jnp.zeros_like(mix)
    top[...] = jnp.full_like(top, NEG)
    gap[...] = lax.rem(lax.broadcasted_iota(jnp.int32, (BLOCK, STRIP), 1), CHIP) - lax.broadcasted_iota(jnp.int32, (BLOCK, STRIP), 0)

    for i in range(4):
        d = order[i]
        q_load(i).wait()
        t = _dot(a[...], w[2 + i])
        dst = qr.at[role] if d == 0 else qs.at[d]
        for g in range(G):
            dst[g * CHIP : (g + 1) * CHIP, :] = turned(t[:, g * HEAD : (g + 1) * HEAD], slice(None))
        wo_load(4 + i).start()
        for n in ((), (1, 2), (3,), ())[i]:
            for h in range(2):
                half_arrived(flip(n), h)
            share(flip(n))
        if d:
            send(qs.at[d], qr.at[role], q_s.at[d - 1], q_r.at[role], at(flip(d), c)).start()

    ones = jnp.ones((8, BLOCK), BF16)

    def items(tasks, masked=False):
        strips = []
        for r, m in tasks:
            halves = [kv[2 * m + i, n] for i in range(2) for n in range(2)]
            keys = jnp.concatenate([h[:OWN] for h in halves], axis=0)
            values = jnp.concatenate([h[OWN:] for h in halves], axis=1)
            values = jnp.concatenate([values, ones], axis=0)
            strips += [(r, keys, values, slice(i, i + STRIP)) for i in range(0, COLS, STRIP)]
        scores = [_dot(keys, qr[r, cols, :], 1, 1) for r, keys, _, cols in strips]
        weights, keeps = [], []
        for (r, _, _, cols), v in zip(strips, scores):
            if masked:
                v = jnp.where(gap[...] >= -CHIP * lax.rem(r, 2), v, HIDDEN)
            old = top[r, 0:1, cols]
            new = jnp.maximum(old, v.max(axis=0, keepdims=True))
            top[r, 0:1, cols] = new
            weights.append(jnp.exp2((v - new) * E).astype(BF16))
            keeps.append(jnp.exp2((old - new) * E))
        for (r, _, values, cols), v, keep in zip(strips, weights, keeps):
            mix[r, :, cols] = mix[r, :, cols] * keep + _dot(values, v)

    y_group, z_group, far_group = (1 - py) * 2 + zh, py * 2 + 1 - zh, (1 - py) * 2 + 1 - zh

    def take(g, xx):
        sent = {"y": (xx == 0) | (py == 1), "z": (xx == 0) | (zh == 1) | (py == 0), "far": (xx == 0) | (py == 1)}[g]
        number = {"y": y_group, "z": z_group, "far": far_group}[g]

        @pl.when(sent)
        def _():
            for n in range(2):
                s = slot(xx * 2 + n, number)
                arrived(s)
                if g == "z":

                    @pl.when(along_y(xx))
                    def _():
                        send(kv.at[s], kv.at[s], f_s.at[s], kv_r.at[s], y_dev).start()

    def q_arrived(r):
        send(qs.at[1], qr.at[r], q_s.at[0], q_r.at[r], partner).wait_recv()

    def counts(r, m):
        return m < lax.div(r, 2) * 4 + group

    def single(r, m):
        @pl.when(counts(r, m))
        def _():
            items([(r, m)])

    def full(n, task):
        lax.fori_loop(0, n, lambda i, _: (single(*task(i)), 0)[1], 0)

    def both(n, task):
        def one(i, _):
            first, second = task(i)

            @pl.when(counts(*second))
            def _():
                items([first, second])

            @pl.when(jnp.logical_not(counts(*second)))
            def _():
                single(*first)

            return 0

        lax.fori_loop(0, n, one, 0)

    def pick(i, *choices):
        got = choices[-1]
        for n in range(len(choices) - 2, -1, -1):
            got = jnp.where(i == n, choices[n], got)
        return got

    def diagonal(r):
        items([(r, lax.div(r, 2) * 4 + group)], True)

    def finish(r):
        o = mix[r, :HEAD, :] * (1 / mix[r, HEAD : HEAD + 1, :])
        for g in range(G):
            for h in range(2):
                first = g * CHIP + h * OWN
                os[r, h, :, g * HEAD : (g + 1) * HEAD] = o[:, first : first + OWN].T.astype(BF16)
        for h in range(2):
            to = at(r, h)

            @pl.when(to != dev)
            def _():
                send(os.at[r, h], orr.at[c * 4 + role], o_s.at[r, h], o_r.at[c * 4 + role], to).start()

            @pl.when(to == dev)
            def _():
                orr[c * 4 + role] = os[r, h]

    beside = flip(2)
    diagonal(role)
    full(1, lambda i: (role, group))

    def beyond(i, _):
        xx = jnp.where(i == 0, px, 1 - px)
        take("y", xx)
        full(1, lambda i: (role, 4 * xx + y_group))
        return 0

    lax.fori_loop(0, 2, beyond, 0)
    for d in range(4):
        share_z(flip(d), 1)
    q_arrived(beside)
    diagonal(beside)
    full(3, lambda i: (beside, pick(i, group, y_group, 4 + y_group)))
    take("z", 0)
    both(1, lambda i: ((2 + zl, z_group), (zl, z_group)))
    take("far", 0)
    both(1, lambda i: ((2 + zl, far_group), (zl, far_group)))
    finish(zl)

    r0, r1 = 1 - zl, 3 - zl

    @pl.when(py == 0)
    def _():
        take("z", 1)

    q_arrived(r0)
    q_arrived(r1)
    items([(r0, group), (r1, 4 + group)], True)
    both(3, lambda i: ((r1, pick(i, y_group, z_group, far_group)), (r0, pick(i, y_group, z_group, far_group))))
    finish(r0)
    both(1, lambda i: ((r1, group), (r1, 4 + y_group)))

    def late(i, _):
        @pl.when((i == 0) & (py == 1))
        def _():
            take("z", 1)

        @pl.when(i == 1)
        def _():
            take("far", 1)

        m = 4 + pick(i, z_group, far_group)

        @pl.when(counts(r1, m))
        def _():
            items([(r1, m), (2 + zl, m)])

        return 0

    lax.fori_loop(0, 2, late, 0)
    lax.fori_loop(0, 2, lambda i, _: (finish(pick(i, r1, 2 + zl)), 0)[1], 0)

    for n in range(8):
        wo_load(n).wait()

    def project(r, last):
        for cc in range(2):
            j = cc * 4 + r

            @pl.when(at(r, cc) != dev)
            def _():
                send(os.at[0, 0], orr.at[j], o_s.at[0, 0], o_r.at[j], partner).wait_recv()

        for n in range(8):
            here = slice(n * PIECE, (n + 1) * PIECE)
            t = acc[:, here]
            for cc in range(2):
                j = cc * 4 + r
                t = t + _dot(orr[j], w[(n + 6) % 8, pl.ds(pl.multiple_of(j * PIECE, PIECE), PIECE), :])
            if last:
                out[:, here] = t.astype(BF16)
            else:
                acc[:, here] = t

    acc[...] = xs[pl.ds(mine, OWN), :].astype(F32)
    lax.fori_loop(0, 3, lambda n, _: (project(flip(pick(n, 0, 1, 3)), False), 0)[1], 0)
    project(flip(2), True)

    x_send.wait_send()
    for d in (1, 2, 3):
        for n in range(2):
            half(d, n).wait_send()
        send(qs.at[d], qr.at[role], q_s.at[d - 1], q_r.at[role], partner).wait_send()

    def left(r, _):
        s, xx = slot(r), lax.div(r, 2)

        @pl.when(along_z(xx))
        def _():
            z_send(s).wait_send()

        @pl.when(along_y(xx))
        def _():
            y_send(s).wait_send()

        came = slot(r, z_group)

        @pl.when(((xx == 0) | (zh == 1) | (py == 0)) & along_y(xx))
        def _():
            send(kv.at[came], kv.at[came], f_s.at[came], kv_r.at[came], y_dev).wait_send()

        for h in range(2):

            @pl.when(at(r, h) != dev)
            def _():
                send(os.at[r, h], orr.at[0], o_s.at[r, h], o_r.at[0], partner).wait_send()

        return 0

    lax.fori_loop(0, 4, left, 0)


def solution(mesh):
    def step(x, gain, wq, wk, wv, wo):
        half = HEAD // 2
        freq = (THETA ** (-np.arange(half, dtype=np.float32) / half)).astype(np.float32)
        freq = jnp.asarray(np.tile(freq, 2)[None])
        vmem, hbm = pl.BlockSpec(memory_space=pltpu.VMEM), pl.BlockSpec(memory_space=pl.ANY)
        dma = pltpu.SemaphoreType.DMA
        return pl.pallas_call(
            _kernel,
            out_shape=pltpu.VMEM((OWN, D), BF16),
            in_specs=[hbm, vmem, vmem, hbm, hbm, hbm, hbm],
            out_specs=vmem,
            scratch_shapes=[
                pltpu.VMEM((8, D, PIECE), BF16),
                pltpu.VMEM((CHIP, D), BF16),
                pltpu.VMEM((CHIP, D), BF16),
                pltpu.VMEM((CHIP, HEAD), F32),
                pltpu.VMEM((CHIP, HEAD), F32),
                pltpu.VMEM((4, 2, CHIP, HEAD), BF16),
                pltpu.VMEM((16, 2, CHIP, HEAD), BF16),
                pltpu.VMEM((4, COLS, HEAD), BF16),
                pltpu.VMEM((4, COLS, HEAD), BF16),
                pltpu.VMEM((4, 8, COLS), F32),
                pltpu.VMEM((4, SUM, COLS), F32),
                pltpu.VMEM((BLOCK, STRIP), jnp.int32),
                pltpu.VMEM((4, 2, OWN, PIECE), BF16),
                pltpu.VMEM((8, OWN, PIECE), BF16),
                pltpu.VMEM((OWN, D), F32),
                dma, dma((6,)), dma((8,)), dma, dma, dma((3, 2)), dma((4, 2)), dma((16,)), dma((16,)), dma((16,)), dma((16,)), dma((3,)), dma((4,)),
                dma((4, 2)), dma((8,)),
            ],
            compiler_params=pltpu.CompilerParams(collective_id=0, has_side_effects=True, vmem_limit_bytes=60 * 2**20),
        )(x, gain, freq, wq, wk, wv, wo)

    tokens, whole = P(("dp", "sp"), None), P(None, None)
    return jax.shard_map(
        step,
        mesh=mesh,
        in_specs=(tokens, P(None), whole, whole, whole, whole),
        out_specs=tokens,
        check_vma=False,
    )
```
